32 devices in a mesh: grp: 16 (over z, y, x), rep: 2 (over core).
Axes of the slice: x: 2, y: 2, z: 4, core: 2. Of those that a mesh axis runs over, the one named last changes fastest.
Arguments:
- vectors: bfloat16 [4096, 768], P(('grp', 'rep')), may hold values from -6 to 6
- list_ids: int32 [4096, 8], P(('grp', 'rep')), may hold values from -1 to 8191, as said below
- spill_weight: int32 [4096, 8], P(('grp', 'rep')), may hold values from 1 to 4
- list_pos: int32 [8192], replicated, may hold values from 0 to 8191, as said below
- old_centroids: float32 [8192, 768], P('grp'), may hold values from -12 to 12
Outputs:
- refined: float32 [8192, 768], P('grp')
- new_dist: float32 [4096, 8], P(('grp', 'rep'))
The draws below stay inside these ranges and needn't reach their ends.
Inputs may be any that keep to these rules, and one draw needn't show every extreme that they name: `list_ids`: entries are list numbers or -1; the lists of one row are distinct. List l is owned by grp index list_pos[l] // 512. Among the rows of one device (aligned blocks of 128 rows), at most 32 slots name lists of one owner, and in every block some owner gets exactly 32. `list_pos`: A permutation of the list numbers.
All inputs are finite; a program needn't handle non-finite values.
Results may differ from the reference program's by a relative error of at most 0.0003.
Values may be sent and summed in bfloat16 or wider, within the bound.
A program may use at most 64 MiB of HBM per device.

```python
import jax
import jax.numpy as jnp
from jax import lax

D = 768
K = 8
V_DEV = 128
LPO = 512
OWNERS = 16
VECS = 4096
LISTS = 8192
CAP = 32


def lists_layout(key):
    list_pos = jax.random.permutation(jax.random.fold_in(key, 11), LISTS).astype(jnp.int32)
    at_position = jnp.argsort(list_pos, stable=True).astype(jnp.int32)
    hot_owner = jax.random.randint(jax.random.fold_in(key, 12), (OWNERS,), 0, 8) == 0
    block_count = VECS // V_DEV
    block_keys = jax.random.split(jax.random.fold_in(key, 13), block_count)

    def one_block(block_key):
        key_one, key_two, key_three, key_four = jax.random.split(block_key, 4)
        counts = jnp.where(hot_owner, CAP, jax.random.randint(key_one, (OWNERS,), CAP // 4, CAP // 2 + 1))
        full_owner = jax.random.randint(key_two, (), 0, OWNERS)
        counts = jnp.where(jnp.arange(OWNERS) == full_owner, CAP, counts)
        owner_of = jnp.repeat(jnp.arange(OWNERS, dtype=jnp.int32), CAP)
        seat_number = jnp.tile(jnp.arange(CAP, dtype=jnp.int32), OWNERS)
        tickets = jnp.where(seat_number < counts[owner_of], owner_of, -1).astype(jnp.int32)
        padding = jnp.full((V_DEV * K - OWNERS * CAP,), -1, jnp.int32)
        tickets = jnp.concatenate([tickets, padding])
        tickets = jax.random.permutation(key_three, tickets).reshape(V_DEV, K)
        column = jnp.arange(K, dtype=jnp.int32)[None, :]
        local_row = column + K * jax.random.randint(key_four, (V_DEV, K), 0, LPO // K)
        position = jnp.maximum(tickets, 0) * LPO + local_row
        return jnp.where(tickets >= 0, at_position[position], -1).astype(jnp.int32)
    list_ids = jax.vmap(one_block)(block_keys).reshape(VECS, K)
    return (list_pos, list_ids)


def draw_list_ids(key, part):
    return lists_layout(key)[1]


def draw_list_pos(key, part):
    return lists_layout(key)[0]


def touch_ends(result, own_key, smallest, top_value):
    index_at = [jax.random.randint(jax.random.fold_in(own_key, axis), (), 0, length) for axis, length in enumerate(result.shape)]
    longest = result.shape.index(max(result.shape))
    next_to = index_at[:longest] + [(index_at[longest] + 1) % result.shape[longest]] + index_at[longest + 1:]
    return result.at[tuple(index_at)].set(smallest).at[tuple(next_to)].set(top_value)


def level_of(own_key, shape, cuts, least, top_value):
    factor_of, own = 1.0, jax.random.fold_in(own_key, 6)
    for dim, parts in cuts:
        draws = jnp.exp(jax.random.uniform(jax.random.fold_in(own, dim), (parts,), jnp.float32, least / len(cuts), top_value / len(cuts)))
        factor_of = factor_of * jnp.repeat(draws, shape[dim] // parts).reshape([-1 if axis == dim else 1 for axis in range(len(shape))])
    return factor_of


def normal_values(key, dims, deviation, bound, shards=(), held_as=jnp.bfloat16):
    array = deviation * jax.random.normal(key, dims, jnp.float32)
    if shards:
        array = array * level_of(key, dims, shards, -0.22, 0.18)
    return jnp.clip(array, -bound, bound).astype(held_as)


def setup_inputs(seed: int = 0) -> dict:
    keys = jax.random.split(jax.random.key(seed), 6)
    vectors = normal_values(keys[0], (VECS, D), 1.0, 6.0, ((0, 32),))
    list_ids = draw_list_ids(jax.random.fold_in(keys[5], 71), 0)
    spill_weight = touch_ends(jax.random.randint(keys[2], (VECS, K), 1, 5), jax.random.fold_in(keys[2], 1), 1, 4).astype(jnp.int32)
    list_pos = draw_list_pos(jax.random.fold_in(keys[5], 71), 0)
    old_centroids = normal_values(keys[4], (LISTS, D), 2.0, 12.0, ((0, 16),), jnp.float32)
    return dict(vectors=vectors, list_ids=list_ids, spill_weight=spill_weight, list_pos=list_pos, old_centroids=old_centroids)


def reference(vectors, list_ids, spill_weight, list_pos, old_centroids):
    block_count = VECS // V_DEV
    is_live = list_ids >= 0
    places = jnp.where(is_live, list_pos[jnp.maximum(list_ids, 0)], 0).astype(jnp.int32)
    weights = jnp.where(is_live, spill_weight.astype(jnp.float32), jnp.float32(0.0))
    vector_blocks = vectors.reshape(block_count, V_DEV, D)
    place_blocks = places.reshape(block_count, V_DEV, K)
    weight_blocks = weights.reshape(block_count, V_DEV, K)

    def accumulate(running, piece_item):
        weighted_sums, totals = running
        rows_in, place_in, weight_in = piece_item
        row_values = rows_in.astype(jnp.float32)
        centre_rows = old_centroids[place_in]
        sq_norms = jnp.sum((row_values[:, None, :] - centre_rows) ** 2, axis=-1)
        shares = weight_in / (1.0 + sq_norms / D)
        flat_places = place_in.reshape(-1)
        weighted_sums = weighted_sums.at[flat_places].add((shares[:, :, None] * row_values[:, None, :]).reshape(-1, D))
        totals = totals.at[flat_places].add(shares.reshape(-1))
        return (weighted_sums, totals), jnp.float32(0.0)

    start_state = (jnp.zeros((LISTS, D), jnp.float32), jnp.zeros((LISTS,), jnp.float32))
    final_state, unused = lax.scan(accumulate, start_state, (vector_blocks, place_blocks, weight_blocks))
    weighted_sums, totals = final_state
    refined = (old_centroids + weighted_sums) / (1.0 + totals[:, None])

    def distance(piece_item):
        rows_in, place_in = piece_item
        row_values = rows_in.astype(jnp.float32)
        return jnp.sum((row_values[:, None, :] - refined[place_in]) ** 2, axis=-1) / D

    spread = lax.map(distance, (vector_blocks, place_blocks)).reshape(VECS, K)
    new_dist = jnp.where(is_live, spread, jnp.float32(0.0))
    return refined, new_dist
```

```python
import functools
import math

import jax
import jax.numpy as jnp
from jax import lax
from jax.experimental import pallas as pl
from jax.experimental.pallas import tpu as pltpu
from jax.sharding import PartitionSpec as P

D = 768


def decode_meta(meta_rows):
    values = meta_rows.astype(jnp.int32)
    tag_value = values[:, 0] * 128 + values[:, 1]
    return (tag_value > 0, jnp.maximum(tag_value - 1, 0), values[:, 2].astype(jnp.float32))


def pick_block(table, index_block):
    table_iota = jnp.arange(table.shape[0], dtype=jnp.int32)
    if table.dtype == jnp.float32:
        selector = (index_block[:, None] == table_iota[None, :]).astype(jnp.float32)
        return jnp.dot(
            selector, table, precision=lax.Precision.HIGHEST, preferred_element_type=jnp.float32
        )
    selector = (index_block[:, None] == table_iota[None, :]).astype(table.dtype)
    return jnp.dot(selector, table, preferred_element_type=jnp.float32).astype(table.dtype)


def pick_rows(table, indices):
    total_rows = indices.shape[0]
    block_rows = math.gcd(512, total_rows)
    block_count = total_rows // block_rows
    picked = lax.map(
        lambda index_block: pick_block(table, index_block), indices.reshape(block_count, block_rows)
    )
    return picked.reshape(total_rows, table.shape[1])


def owner_sums(rows_all, slot_all, weight_all, old_centroids, lists_here):
    total_rows, feature_dim = rows_all.shape
    block_rows = math.gcd(512, total_rows)
    block_count = total_rows // block_rows
    row_blocks = rows_all.reshape(block_count, block_rows, feature_dim)
    slot_blocks = slot_all.reshape(block_count, block_rows)
    weight_blocks = weight_all.reshape(block_count, block_rows)
    list_iota = jnp.arange(lists_here, dtype=jnp.int32)

    def accumulate(running, piece_item):
        weighted_sums, totals = running
        rows_in, slot_in, weight_in = piece_item
        row_values = rows_in.astype(jnp.float32)
        centre_rows = pick_block(old_centroids, slot_in)
        sq_norms = jnp.sum((row_values - centre_rows) ** 2, axis=-1)
        shares = weight_in / (1.0 + sq_norms / D)
        placed = (slot_in[None, :] == list_iota[:, None]).astype(jnp.float32) * shares[None, :]
        weighted_sums = weighted_sums + jnp.dot(
            placed, row_values, precision=lax.Precision.HIGHEST, preferred_element_type=jnp.float32
        )
        totals = totals + jnp.sum(placed, axis=1)
        return ((weighted_sums, totals), jnp.float32(0.0))

    start_state = (
        jnp.zeros((lists_here, feature_dim), jnp.float32),
        jnp.zeros((lists_here,), jnp.float32),
    )
    final_state, unused = lax.scan(
        accumulate, start_state, (row_blocks, slot_blocks, weight_blocks)
    )
    return final_state


def shards_general(vectors, list_ids, spill_weight, list_pos, old_centroids):
    owners = lax.axis_size("grp")
    row_count, slot_count = list_ids.shape
    feature_dim = vectors.shape[1]
    lists_here = old_centroids.shape[0]
    cap_slots = row_count * slot_count // (2 * owners)
    seat_total = owners * cap_slots
    pair_count = row_count * slot_count
    is_live = list_ids >= 0
    places = jnp.where(is_live, list_pos[jnp.maximum(list_ids, 0)], 0)
    target = jnp.where(is_live, places // lists_here, owners).reshape(-1)
    sorted_order = jnp.argsort(target, stable=True)
    ranked = target[sorted_order]
    counts = jnp.sum(
        (target[:, None] == jnp.arange(owners, dtype=jnp.int32)[None, :]).astype(jnp.int32), axis=0
    )
    starts = jnp.concatenate([jnp.cumsum(counts) - counts, jnp.zeros((1,), jnp.int32)])
    within = jnp.arange(pair_count, dtype=jnp.int32) - starts[ranked]
    seat_sorted = jnp.where(ranked < owners, ranked * cap_slots + within, seat_total)
    seat_index = jnp.zeros((pair_count,), jnp.int32).at[sorted_order].set(seat_sorted)
    pair_of_seat = (
        jnp.full((seat_total,), -1, jnp.int32)
        .at[seat_index]
        .set(jnp.arange(pair_count, dtype=jnp.int32), mode="drop")
    )
    filled = pair_of_seat >= 0
    pair_safe = jnp.maximum(pair_of_seat, 0)
    source_row = jnp.where(filled, pair_safe // slot_count, -1)
    send_rows = pick_rows(vectors, source_row)
    local_flat = (places % lists_here).reshape(-1)
    weight_flat = spill_weight.reshape(-1)
    tag_out = jnp.where(filled, local_flat[pair_safe] + 1, 0)
    weight_out = jnp.where(filled, weight_flat[pair_safe], 0)
    send_meta = jnp.stack([tag_out // 128, tag_out % 128, weight_out], axis=-1).astype(jnp.bfloat16)
    got_rows, got_meta = (
        lax.all_to_all(
            send_rows.reshape(owners, cap_slots, feature_dim),
            "grp",
            split_axis=0,
            concat_axis=0,
            tiled=True,
        ),
        lax.all_to_all(
            send_meta.reshape(owners, cap_slots, 3), "grp", split_axis=0, concat_axis=0, tiled=True
        ),
    )
    got_rows = got_rows.reshape(seat_total, feature_dim)
    got_meta = got_meta.reshape(seat_total, 3)
    seat_live, seat_row, seat_weight = decode_meta(got_meta)
    weighted_sums, totals = owner_sums(got_rows, seat_row, seat_weight, old_centroids, lists_here)
    weighted_sums, totals = lax.psum((weighted_sums, totals), "rep")
    refined = (old_centroids + weighted_sums) / (1.0 + totals[:, None])
    block_rows = math.gcd(512, seat_total)
    block_count = seat_total // block_rows
    row_blocks = got_rows.reshape(block_count, block_rows, feature_dim)
    slot_blocks = seat_row.reshape(block_count, block_rows)

    def distance(piece_item):
        rows_in, slot_in = piece_item
        row_values = rows_in.astype(jnp.float32)
        return jnp.sum((row_values - pick_block(refined, slot_in)) ** 2, axis=-1) / D

    owner_dist = lax.map(distance, (row_blocks, slot_blocks)).reshape(owners, cap_slots)
    seat_dist = lax.all_to_all(owner_dist, "grp", split_axis=0, concat_axis=0, tiled=True).reshape(
        seat_total
    )
    picked = seat_dist[jnp.minimum(seat_index, seat_total - 1)].reshape(row_count, slot_count)
    new_dist = jnp.where(is_live, picked, jnp.float32(0.0))
    return (refined, new_dist)


MESH = pl.DeviceIdType.MESH
LANES = 128
CHUNKS = 1
F32 = jnp.float32
BF16 = jnp.bfloat16


def xor_index(a, b_const, bits):
    out = 0
    for i in range(bits):
        bit = (a // (1 << i)) % 2
        out = out + ((1 - bit) if (b_const >> i) & 1 else bit) * (1 << i)
    return out


def split_two(x):
    hi = x.astype(BF16)
    return hi, (x - hi.astype(F32)).astype(BF16)


def dot(a, b):
    return jnp.dot(a, b, preferred_element_type=F32)


def iota(shape, dim):
    return lax.broadcasted_iota(jnp.int32, shape, dim)


def fused_kernel(
    owners, cap,
    vec_ref, ids_ref, weight_ref, pos_ref, cent_hbm,
    refined_ref, dist_ref,
    cent, cent_hi, cent_lo, send_buf, meta_send, rows, metas, sib_rows, sib_metas,
    acc, tot, back_send, back, send_up, up_rows, sib_up, raw_in, seat_out, seat_in, up_mask, up_placed,
    local_sem, s_raw, r_raw, s_seat, r_seat, s_up, r_up, s_fup, r_fup, s_rows, r_rows, s_meta, r_meta, s_fwd, r_fwd, s_fmeta, r_fmeta, s_back, r_back,
):
    me = lax.axis_index("grp")
    rep = lax.axis_index("rep")
    bits = owners.bit_length() - 1
    row_count, feature_dim = vec_ref.shape
    slot_count = ids_ref.shape[0]
    lists_here = cent.shape[0]
    groups = owners * cap // LANES
    per_group = owners // groups
    upper = owners // 2
    half_groups = groups // 2
    up_seats = upper * cap
    chunk = feature_dim // CHUNKS
    peers = [xor_index(me, j, bits) for j in range(owners)]

    barrier = pltpu.get_barrier_semaphore()
    for j in range(1, owners):
        pl.semaphore_signal(barrier, inc=1, device_id={"grp": peers[j]}, device_id_type=MESH)
    pl.semaphore_signal(barrier, inc=1, device_id={"rep": 1 - rep}, device_id_type=MESH)
    cent_copy = pltpu.make_async_copy(cent_hbm, cent, local_sem)
    cent_copy.start()

    def raw_copy(c):
        span = pl.ds(c * chunk, chunk)
        return pltpu.make_async_remote_copy(
            src_ref=vec_ref.at[:, span], dst_ref=raw_in.at[c], send_sem=s_raw.at[c],
            recv_sem=r_raw.at[c], device_id={"grp": peers[upper]}, device_id_type=MESH,
        )

    pl.semaphore_wait(barrier, owners)
    for c in range(CHUNKS):
        raw_copy(c).start()

    table = pos_ref[...]
    table_rows = table.shape[0]
    raw_ids = ids_ref[...]
    safe_ids = jnp.maximum(raw_ids, 0)
    found = jnp.zeros((slot_count, row_count), jnp.int32)
    for r in range(table_rows):
        line = jnp.broadcast_to(table[r : r + 1], (slot_count, LANES))
        taken = jnp.take_along_axis(line, safe_ids % LANES, axis=1, mode="promise_in_bounds")
        found = jnp.where(safe_ids // LANES == r, taken, found)
    ids = jnp.transpose(raw_ids)
    weights = jnp.transpose(weight_ref[...])
    places = jnp.transpose(found)
    lane = iota((row_count, LANES), 1)
    id_cols = [ids[:, k : k + 1] for k in range(slot_count)]
    live_cols, owner_cols, code_cols = [], [], []
    for k in range(slot_count):
        c = id_cols[k]
        place = places[:, k : k + 1]
        owner = place // lists_here
        live_cols.append(c >= 0)
        owner_cols.append(jnp.where(c >= 0, owner ^ me, -1))
        code_cols.append(((place % lists_here) * 8 + weights[:, k : k + 1]).astype(F32))

    member = [(lane == o) for o in owner_cols]
    ones = [m.astype(F32) for m in member]
    lower = (iota((row_count, row_count), 0) > iota((row_count, row_count), 1)).astype(F32).astype(BF16)
    before = dot(lower, jnp.concatenate(ones, axis=1).astype(BF16))
    base = jnp.zeros((1, LANES), F32)
    seats_lane = jnp.full((row_count, LANES), -1.0, F32)
    seat_cols = []
    for k in range(slot_count):
        inside = before[:, k * LANES : (k + 1) * LANES] + base
        rank = jnp.sum(jnp.where(member[k], inside, 0.0), axis=1, keepdims=True)
        base = base + jnp.sum(ones[k], axis=0, keepdims=True)
        seat = jnp.where(live_cols[k], owner_cols[k].astype(F32) * cap + rank, -1.0)
        seat_cols.append(seat)
        seats_lane = jnp.where(lane == k, seat, seats_lane)
    seat_rows = jnp.transpose(seats_lane)
    seat_out[...] = seat_rows[:slot_count]

    seat_copy = pltpu.make_async_remote_copy(
        src_ref=seat_out, dst_ref=seat_in, send_sem=s_seat, recv_sem=r_seat,
        device_id={"grp": peers[upper]}, device_id_type=MESH,
    )

    def relay_copy(c, j):
        return pltpu.make_async_remote_copy(
            src_ref=send_up.at[c, j], dst_ref=up_rows.at[c, j],
            send_sem=s_up.at[c, j], recv_sem=r_up.at[c, j],
            device_id={"grp": peers[j]}, device_id_type=MESH,
        )

    def forward_up(c, h):
        part = pl.ds(h * (upper // 2), upper // 2)
        return pltpu.make_async_remote_copy(
            src_ref=up_rows.at[c, part], dst_ref=sib_up.at[c, part],
            send_sem=s_fup.at[c, h], recv_sem=r_fup.at[c, h],
            device_id={"rep": 1 - rep}, device_id_type=MESH,
        )

    seat_copy.start()

    for g in range(groups):
        q = (lane + g * LANES).astype(F32)
        code = jnp.zeros((row_count, LANES), F32)
        for k in range(slot_count):
            code = code + jnp.where(seat_cols[k] == q, code_cols[k], 0.0)
        meta_send[g] = jnp.sum(code, axis=0, keepdims=True)

    vectors = vec_ref[...]

    def row_copy(j):
        return pltpu.make_async_remote_copy(
            src_ref=send_buf.at[j], dst_ref=rows.at[j], send_sem=s_rows.at[j], recv_sem=r_rows.at[j],
            device_id={"grp": peers[j]}, device_id_type=MESH,
        )

    def meta_copy(j):
        return pltpu.make_async_remote_copy(
            src_ref=meta_send.at[j // per_group], dst_ref=metas.at[j], send_sem=s_meta.at[j],
            recv_sem=r_meta.at[j], device_id={"grp": peers[j]}, device_id_type=MESH,
        )

    def back_copy(j):
        return pltpu.make_async_remote_copy(
            src_ref=back_send.at[j // per_group], dst_ref=back.at[j], send_sem=s_back.at[j],
            recv_sem=r_back.at[j], device_id={"grp": peers[j]}, device_id_type=MESH,
        )

    def forward_copy(g):
        span = pl.ds(g * per_group, per_group)
        return pltpu.make_async_remote_copy(
            src_ref=rows.at[span], dst_ref=sib_rows.at[span], send_sem=s_fwd.at[g], recv_sem=r_fwd.at[g],
            device_id={"rep": 1 - rep}, device_id_type=MESH,
        )

    def forward_meta(g):
        span = pl.ds(g * per_group, per_group)
        return pltpu.make_async_remote_copy(
            src_ref=metas.at[span], dst_ref=sib_metas.at[span], send_sem=s_fmeta.at[g],
            recv_sem=r_fmeta.at[g], device_id={"rep": 1 - rep}, device_id_type=MESH,
        )

    for j in reversed(range(1, owners)):
        meta_copy(j).start()
    metas[0] = meta_send[0]

    def pick_rows_of(seat_table, first, count, values):
        q = (iota((count, row_count), 0) + first).astype(F32)
        pick = jnp.zeros((count, row_count), F32)
        for k in range(slot_count):
            pick = pick + (seat_table[k : k + 1, :] == q).astype(F32)
        pick = pick.astype(BF16)
        return pick if values is None else dot(pick, values).astype(BF16)

    picked = pick_rows_of(seat_rows, 0, up_seats, vectors).reshape(upper, cap, feature_dim)
    send_buf[pl.ds(0, upper)] = picked
    rows[0] = picked[0]
    for j in reversed(range(1, upper)):
        row_copy(j).start()

    cent_copy.wait()
    hi, lo = split_two(cent[...])
    cent_hi[...] = hi
    cent_lo[...] = lo
    acc[...] = cent[...]
    tot[...] = jnp.zeros_like(tot)

    lane_row = iota((1, LANES), 1)

    def meta_row(ref, g):
        out = ref[g * per_group]
        for b in range(1, per_group):
            out = jnp.where(lane_row // cap == b, ref[g * per_group + b], out)
        return out

    def codes_of(own, g):
        row = meta_row(metas if own else sib_metas, g).astype(jnp.int32)
        col = jnp.transpose(jnp.broadcast_to(row, (LANES, LANES)))
        return row, col

    def gather_mask(col):
        wide = jnp.concatenate([col // 8] * (lists_here // LANES), axis=1)
        return (wide == iota((LANES, lists_here), 1)).astype(F32).astype(BF16)

    def shares_of(weight, sq):
        share = weight / (1.0 + sq / feature_dim)
        count = share.shape[0]
        hi_part = share.astype(BF16).astype(F32)
        at = iota((count, LANES), 1)
        two = jnp.where(at == 0, hi_part, jnp.where(at == 1, share - hi_part, 0.0))
        return share, two.astype(BF16)

    def lower_group(g):
        for j in range(max(g * per_group, 1), (g + 1) * per_group):
            meta_copy(j).wait_recv()
            row_copy(j).wait_recv()
        forward_meta(g).start()
        forward_copy(g).start()
        row_a, col_a = codes_of(True, g)
        mask_a = gather_mask(col_a)
        span = pl.ds(g * per_group, per_group)
        forward_meta(g).wait_recv()
        row_b, col_b = codes_of(False, g)
        mask_b = gather_mask(col_b)
        mask = jnp.concatenate([mask_a, mask_b], axis=0)
        centre = dot(mask, cent_hi[...]) + dot(mask, cent_lo[...])
        forward_copy(g).wait_recv()
        got = jnp.concatenate(
            [rows[span].reshape(LANES, feature_dim), sib_rows[span].reshape(LANES, feature_dim)], axis=0
        ).astype(F32)
        weight = jnp.concatenate([col_a[:, :1] % 8, col_b[:, :1] % 8], axis=0).astype(F32)
        diff = got - centre
        share, share_two = shares_of(weight, jnp.sum(diff * diff, axis=1, keepdims=True))
        sv_hi, sv_lo = split_two(share * got)
        both = jnp.concatenate([row_a, row_b], axis=1) // 8
        placed = (both == iota((lists_here, 2 * LANES), 0)).astype(F32).astype(BF16)
        acc[...] += dot(placed, sv_hi) + dot(placed, sv_lo)
        tot[...] += dot(placed, share_two)

    seat_copy.wait_recv()
    mirror_pick = pick_rows_of(seat_in[...], up_seats, up_seats, None)

    def relay(c):
        raw_copy(c).wait_recv()
        part = dot(mirror_pick, raw_in[c]).astype(BF16).reshape(upper, cap, chunk)
        send_up[c] = part
        up_rows[c, 0] = part[0]
        for j in reversed(range(1, upper)):
            relay_copy(c, j).start()

    up_weights = []

    def upper_codes():
        for g in range(half_groups, groups):
            for j in range(g * per_group, (g + 1) * per_group):
                meta_copy(j).wait_recv()
            forward_meta(g).start()
        for own in (True, False):
            for g in range(half_groups, groups):
                if not own:
                    forward_meta(g).wait_recv()
                row, col = codes_of(own, g)
                at = (0 if own else up_seats) + (g - half_groups) * LANES
                up_mask[pl.ds(at, LANES)] = gather_mask(col)
                up_placed[:, pl.ds(at, LANES)] = (
                    (row // 8 == iota((lists_here, LANES), 0)).astype(F32).astype(BF16)
                )
                up_weights.append((col[:, :1] % 8).astype(F32))

    for c in range(CHUNKS):
        relay(c)
        if c == 0:
            lower_group(0)
    for g in range(1, half_groups):
        lower_group(g)
    upper_codes()

    def up_part(ref, c):
        return ref[c].reshape(up_seats, chunk).astype(F32)

    sq = [jnp.zeros((up_seats, 1), F32), jnp.zeros((up_seats, 1), F32)]
    for c in range(CHUNKS):
        span = pl.ds(c * chunk, chunk)
        for h in range(2):
            for j in range(max(h * (upper // 2), 1), (h + 1) * (upper // 2)):
                relay_copy(c, j).wait_recv()
            forward_up(c, h).start()
        centre = dot(up_mask[...], cent_hi[:, span]) + dot(up_mask[...], cent_lo[:, span])
        diff = up_part(up_rows, c) - centre[:up_seats]
        sq[0] = sq[0] + jnp.sum(diff * diff, axis=1, keepdims=True)
        for h in range(2):
            forward_up(c, h).wait_recv()
        diff = up_part(sib_up, c) - centre[up_seats:]
        sq[1] = sq[1] + jnp.sum(diff * diff, axis=1, keepdims=True)
    share, share_two = shares_of(jnp.concatenate(up_weights, axis=0), jnp.concatenate(sq, axis=0))
    tot[...] += dot(up_placed[...], share_two)
    for c in range(CHUNKS):
        span = pl.ds(c * chunk, chunk)
        got = jnp.concatenate([up_part(up_rows, c), up_part(sib_up, c)], axis=0)
        sv_hi, sv_lo = split_two(share * got)
        acc[:, span] += dot(up_placed[...], sv_hi) + dot(up_placed[...], sv_lo)

    scale = 1.0 / (1.0 + jnp.sum(tot[...], axis=1, keepdims=True))
    refined = acc[...] * scale
    refined_ref[...] = refined
    hi, lo = split_two(refined)
    cent_hi[...] = hi
    cent_lo[...] = lo
    for g in reversed(range(groups)):
        _, col = codes_of(True, g)
        mask = gather_mask(col)
        centre = dot(mask, cent_hi[...]) + dot(mask, cent_lo[...])
        if g < half_groups:
            got = rows[pl.ds(g * per_group, per_group)].reshape(LANES, feature_dim)
        else:
            span = pl.ds((g - half_groups) * per_group, per_group)
            got = jnp.concatenate(
                [up_rows[c, span].reshape(LANES, chunk) for c in range(CHUNKS)], axis=1
            )
        got = got.astype(F32)
        diff = got - centre
        value = jnp.sum(diff * diff, axis=1, keepdims=True) / feature_dim
        back_send[g] = jnp.transpose(jnp.broadcast_to(value, (LANES, LANES)))[:1]
        if g == 0:
            back[0] = back_send[0]
        for j in range(max(g * per_group, 1), (g + 1) * per_group):
            back_copy(j).start()

    seats_int = seat_out[...].astype(jnp.int32)
    for j in range(1, owners):
        back_copy(j).wait_recv()
    spread = [meta_row(back, g) for g in range(groups)]
    out = jnp.zeros((slot_count, row_count), F32)
    for g in range(groups):
        line = jnp.broadcast_to(spread[g], (slot_count, LANES))
        at = jnp.maximum(seats_int, 0) % LANES
        taken = jnp.take_along_axis(line, at, axis=1, mode="promise_in_bounds")
        out = jnp.where((seats_int >= 0) & (seats_int // LANES == g), taken, out)
    dist_ref[...] = out

    for j in range(1, owners):
        meta_copy(j).wait_send()
        back_copy(j).wait_send()
    for j in range(1, upper):
        row_copy(j).wait_send()
    for c in range(CHUNKS):
        raw_copy(c).wait_send()
        for h in range(2):
            forward_up(c, h).wait_send()
        for j in range(1, upper):
            relay_copy(c, j).wait_send()
    seat_copy.wait_send()
    for g in range(groups):
        forward_meta(g).wait_send()
    for g in range(half_groups):
        forward_copy(g).wait_send()


def shards(vectors, list_ids, spill_weight, list_pos, old_centroids):
    owners = lax.axis_size("grp")
    row_count, slot_count = list_ids.shape
    feature_dim = vectors.shape[1]
    lists_here = old_centroids.shape[0]
    cap = row_count * slot_count // (2 * owners)
    if cap % 16 or LANES % cap or row_count != LANES or owners & (owners - 1) or lists_here % LANES or owners * cap % (2 * LANES):
        return shards_general(vectors, list_ids, spill_weight, list_pos, old_centroids)
    if feature_dim % (CHUNKS * LANES):
        return shards_general(vectors, list_ids, spill_weight, list_pos, old_centroids)
    groups = owners * cap // LANES
    vmem = pl.BlockSpec(memory_space=pltpu.VMEM)
    dma = pltpu.SemaphoreType.DMA
    refined, dist = pl.pallas_call(
        functools.partial(fused_kernel, owners, cap),
        out_shape=(
            pltpu.VMEM((lists_here, feature_dim), F32),
            pltpu.VMEM((slot_count, row_count), F32),
        ),
        in_specs=[vmem, vmem, vmem, vmem, pl.BlockSpec(memory_space=pl.ANY)],
        out_specs=(vmem, vmem),
        scratch_shapes=[
            pltpu.VMEM((lists_here, feature_dim), F32),
            pltpu.VMEM((lists_here, feature_dim), BF16),
            pltpu.VMEM((lists_here, feature_dim), BF16),
            pltpu.VMEM((owners // 2, cap, feature_dim), BF16),
            pltpu.VMEM((groups, 1, LANES), F32),
            pltpu.VMEM((owners // 2, cap, feature_dim), BF16),
            pltpu.VMEM((owners, 1, LANES), F32),
            pltpu.VMEM((owners // 2, cap, feature_dim), BF16),
            pltpu.VMEM((owners, 1, LANES), F32),
            pltpu.VMEM((lists_here, feature_dim), F32),
            pltpu.VMEM((lists_here, LANES), F32),
            pltpu.VMEM((groups, 1, LANES), F32),
            pltpu.VMEM((owners, 1, LANES), F32),
            pltpu.VMEM((CHUNKS, owners // 2, cap, feature_dim // CHUNKS), BF16),
            pltpu.VMEM((CHUNKS, owners // 2, cap, feature_dim // CHUNKS), BF16),
            pltpu.VMEM((CHUNKS, owners // 2, cap, feature_dim // CHUNKS), BF16),
            pltpu.VMEM((CHUNKS, row_count, feature_dim // CHUNKS), BF16),
            pltpu.VMEM((slot_count, row_count), F32),
            pltpu.VMEM((slot_count, row_count), F32),
            pltpu.VMEM((owners * cap, lists_here), BF16),
            pltpu.VMEM((lists_here, owners * cap), BF16),
            dma(()),
            dma((CHUNKS,)), dma((CHUNKS,)), dma(()), dma(()),
            dma((CHUNKS, owners // 2)), dma((CHUNKS, owners // 2)), dma((CHUNKS, 2)), dma((CHUNKS, 2)),
            dma((owners,)), dma((owners,)), dma((owners,)), dma((owners,)),
            dma((groups,)), dma((groups,)), dma((groups,)), dma((groups,)),
            dma((owners,)), dma((owners,)),
        ],
        compiler_params=pltpu.CompilerParams(collective_id=0, has_side_effects=True),
    )(vectors, list_ids.T, spill_weight.T, list_pos.reshape(-1, LANES), old_centroids)
    return refined, dist.T


def solution(mesh):
    return jax.shard_map(
        shards,
        mesh=mesh,
        in_specs=(
            P(("grp", "rep"), None),
            P(("grp", "rep"), None),
            P(("grp", "rep"), None),
            P(),
            P("grp", None),
        ),
        out_specs=(P("grp", None), P(("grp", "rep"), None)),
        check_vma=False,
    )
```

```python
import functools
import math

import jax
import jax.numpy as jnp
from jax import lax
from jax.experimental import pallas as pl
from jax.experimental.pallas import tpu as pltpu
from jax.sharding import PartitionSpec as P

D = 768


def decode_meta(meta_rows):
    values = meta_rows.astype(jnp.int32)
    tag_value = values[:, 0] * 128 + values[:, 1]
    return (tag_value > 0, jnp.maximum(tag_value - 1, 0), values[:, 2].astype(jnp.float32))


def pick_block(table, index_block):
    table_iota = jnp.arange(table.shape[0], dtype=jnp.int32)
    if table.dtype == jnp.float32:
        selector = (index_block[:, None] == table_iota[None, :]).astype(jnp.float32)
        return jnp.dot(
            selector, table, precision=lax.Precision.HIGHEST, preferred_element_type=jnp.float32
        )
    selector = (index_block[:, None] == table_iota[None, :]).astype(table.dtype)
    return jnp.dot(selector, table, preferred_element_type=jnp.float32).astype(table.dtype)


def pick_rows(table, indices):
    total_rows = indices.shape[0]
    block_rows = math.gcd(512, total_rows)
    block_count = total_rows // block_rows
    picked = lax.map(
        lambda index_block: pick_block(table, index_block), indices.reshape(block_count, block_rows)
    )
    return picked.reshape(total_rows, table.shape[1])


def owner_sums(rows_all, slot_all, weight_all, old_centroids, lists_here):
    total_rows, feature_dim = rows_all.shape
    block_rows = math.gcd(512, total_rows)
    block_count = total_rows // block_rows
    row_blocks = rows_all.reshape(block_count, block_rows, feature_dim)
    slot_blocks = slot_all.reshape(block_count, block_rows)
    weight_blocks = weight_all.reshape(block_count, block_rows)
    list_iota = jnp.arange(lists_here, dtype=jnp.int32)

    def accumulate(running, piece_item):
        weighted_sums, totals = running
        rows_in, slot_in, weight_in = piece_item
        row_values = rows_in.astype(jnp.float32)
        centre_rows = pick_block(old_centroids, slot_in)
        sq_norms = jnp.sum((row_values - centre_rows) ** 2, axis=-1)
        shares = weight_in / (1.0 + sq_norms / D)
        placed = (slot_in[None, :] == list_iota[:, None]).astype(jnp.float32) * shares[None, :]
        weighted_sums = weighted_sums + jnp.dot(
            placed, row_values, precision=lax.Precision.HIGHEST, preferred_element_type=jnp.float32
        )
        totals = totals + jnp.sum(placed, axis=1)
        return ((weighted_sums, totals), jnp.float32(0.0))

    start_state = (
        jnp.zeros((lists_here, feature_dim), jnp.float32),
        jnp.zeros((lists_here,), jnp.float32),
    )
    final_state, unused = lax.scan(
        accumulate, start_state, (row_blocks, slot_blocks, weight_blocks)
    )
    return final_state


def shards_general(vectors, list_ids, spill_weight, list_pos, old_centroids):
    owners = lax.axis_size("grp")
    row_count, slot_count = list_ids.shape
    feature_dim = vectors.shape[1]
    lists_here = old_centroids.shape[0]
    cap_slots = row_count * slot_count // (2 * owners)
    seat_total = owners * cap_slots
    pair_count = row_count * slot_count
    is_live = list_ids >= 0
    places = jnp.where(is_live, list_pos[jnp.maximum(list_ids, 0)], 0)
    target = jnp.where(is_live, places // lists_here, owners).reshape(-1)
    sorted_order = jnp.argsort(target, stable=True)
    ranked = target[sorted_order]
    counts = jnp.sum(
        (target[:, None] == jnp.arange(owners, dtype=jnp.int32)[None, :]).astype(jnp.int32), axis=0
    )
    starts = jnp.concatenate([jnp.cumsum(counts) - counts, jnp.zeros((1,), jnp.int32)])
    within = jnp.arange(pair_count, dtype=jnp.int32) - starts[ranked]
    seat_sorted = jnp.where(ranked < owners, ranked * cap_slots + within, seat_total)
    seat_index = jnp.zeros((pair_count,), jnp.int32).at[sorted_order].set(seat_sorted)
    pair_of_seat = (
        jnp.full((seat_total,), -1, jnp.int32)
        .at[seat_index]
        .set(jnp.arange(pair_count, dtype=jnp.int32), mode="drop")
    )
    filled = pair_of_seat >= 0
    pair_safe = jnp.maximum(pair_of_seat, 0)
    source_row = jnp.where(filled, pair_safe // slot_count, -1)
    send_rows = pick_rows(vectors, source_row)
    local_flat = (places % lists_here).reshape(-1)
    weight_flat = spill_weight.reshape(-1)
    tag_out = jnp.where(filled, local_flat[pair_safe] + 1, 0)
    weight_out = jnp.where(filled, weight_flat[pair_safe], 0)
    send_meta = jnp.stack([tag_out // 128, tag_out % 128, weight_out], axis=-1).astype(jnp.bfloat16)
    got_rows, got_meta = (
        lax.all_to_all(
            send_rows.reshape(owners, cap_slots, feature_dim),
            "grp",
            split_axis=0,
            concat_axis=0,
            tiled=True,
        ),
        lax.all_to_all(
            send_meta.reshape(owners, cap_slots, 3), "grp", split_axis=0, concat_axis=0, tiled=True
        ),
    )
    got_rows = got_rows.reshape(seat_total, feature_dim)
    got_meta = got_meta.reshape(seat_total, 3)
    seat_live, seat_row, seat_weight = decode_meta(got_meta)
    weighted_sums, totals = owner_sums(got_rows, seat_row, seat_weight, old_centroids, lists_here)
    weighted_sums, totals = lax.psum((weighted_sums, totals), "rep")
    refined = (old_centroids + weighted_sums) / (1.0 + totals[:, None])
    block_rows = math.gcd(512, seat_total)
    block_count = seat_total // block_rows
    row_blocks = got_rows.reshape(block_count, block_rows, feature_dim)
    slot_blocks = seat_row.reshape(block_count, block_rows)

    def distance(piece_item):
        rows_in, slot_in = piece_item
        row_values = rows_in.astype(jnp.float32)
        return jnp.sum((row_values - pick_block(refined, slot_in)) ** 2, axis=-1) / D

    owner_dist = lax.map(distance, (row_blocks, slot_blocks)).reshape(owners, cap_slots)
    seat_dist = lax.all_to_all(owner_dist, "grp", split_axis=0, concat_axis=0, tiled=True).reshape(
        seat_total
    )
    picked = seat_dist[jnp.minimum(seat_index, seat_total - 1)].reshape(row_count, slot_count)
    new_dist = jnp.where(is_live, picked, jnp.float32(0.0))
    return (refined, new_dist)


MESH = pl.DeviceIdType.MESH
LANES = 128
LINE = 4
F32 = jnp.float32
BF16 = jnp.bfloat16


def xor_index(a, b_const, bits):
    out = 0
    for i in range(bits):
        bit = (a // (1 << i)) % 2
        out = out + ((1 - bit) if (b_const >> i) & 1 else bit) * (1 << i)
    return out


def split_two(x):
    hi = x.astype(BF16)
    return hi, (x - hi.astype(F32)).astype(BF16)


def dot(a, b):
    return jnp.dot(a, b, preferred_element_type=F32)


def iota(shape, dim):
    return lax.broadcasted_iota(jnp.int32, shape, dim)


def take_lanes(line, at):
    wide = jnp.broadcast_to(line, at.shape)
    return jnp.take_along_axis(wide, at, axis=1, mode="promise_in_bounds")


def line_kernel(
    owners, cap,
    vec_hbm, ids_hbm, weight_hbm, pos_hbm, cent_hbm,
    refined_ref, dist_ref,
    ints, vec_other, cent, cent_cat, raw_in, meta_in, seat_keep, send_buf, rows, codes,
    masks, placed, sq_own, sq_sib, acc, tot, back_send, back,
    l_sem, s_own, s_meta, r_raw, r_meta, s_row, r_row, s_code, r_code, s_sq, r_sq, s_back, r_back, s_ref, r_ref,
):
    me = lax.axis_index("grp")
    rep = lax.axis_index("rep")
    slot_count, row_count = seat_keep.shape
    lists_here, half = cent.shape
    table_rows = pos_hbm.shape[0]
    plane = owners // LINE
    pbits = plane.bit_length() - 1
    z = me // plane
    p = me % plane
    mid = ((z + 1) // 2) % 2
    near = z + 1 - 2 * (z % 2)
    inner = LINE - 1 - z
    cross = (z + 2) % LINE
    z_of = [z, near, mid * inner + (1 - mid) * cross, mid * cross + (1 - mid) * inner]
    xz_of = [0, 1, 2 + mid, 3 - mid]
    rep_of = [rep, 1 - rep]
    mine = pl.ds(pl.multiple_of(rep * half, LANES), half)
    theirs = pl.ds(pl.multiple_of((1 - rep) * half, LANES), half)

    def at(place, xp):
        return place * plane + xor_index(p, xp, pbits)

    barrier = pltpu.get_barrier_semaphore()

    def greet(place, xp, r):
        pl.semaphore_signal(barrier, inc=1, device_id={"grp": at(place, xp), "rep": r}, device_id_type=MESH)

    greet(near, 0, 0)
    greet(near, 0, 1)

    @pl.when(mid == 1)
    def _():
        greet(inner, 0, 0)
        greet(inner, 0, 1)

    for j in range(1, plane):
        greet(z, j, rep)
    greet(z, 0, 1 - rep)

    local = [
        pltpu.make_async_copy(vec_hbm.at[:, mine], raw_in.at[0, 0], l_sem.at[0]),
        pltpu.make_async_copy(vec_hbm.at[:, theirs], vec_other, l_sem.at[1]),
        pltpu.make_async_copy(ids_hbm, ints.at[pl.ds(0, slot_count)], l_sem.at[2]),
        pltpu.make_async_copy(weight_hbm, ints.at[pl.ds(slot_count, slot_count)], l_sem.at[2]),
        pltpu.make_async_copy(pos_hbm, ints.at[pl.ds(2 * slot_count, table_rows)], l_sem.at[2]),
        pltpu.make_async_copy(cent_hbm.at[:, mine], cent, l_sem.at[3]),
    ]
    for copy in local:
        copy.start()

    def remote(src, dst, send, recv, place, xp, r):
        return pltpu.make_async_remote_copy(
            src_ref=src, dst_ref=dst, send_sem=send, recv_sem=recv,
            device_id={"grp": at(place, xp), "rep": r}, device_id_type=MESH,
        )

    own_place = [z, near, inner]
    others = pl.ds(1, plane - 1)

    def own_raw(s, f):
        src = raw_in.at[0, 0] if f == 0 else vec_other
        return remote(src, raw_in.at[s, f], s_own.at[s // 2], r_raw.at[s, f], own_place[s], 0, rep_of[f])

    def own_meta(s, f):
        return remote(
            meta_in.at[0, 0], meta_in.at[s, f], s_meta.at[s // 2], r_meta.at[s, f], own_place[s], 0, rep_of[f]
        )

    forward_to = {1: (3, inner), 2: (2, near), 3: (3, near)}

    def forward(s, f):
        to, place = forward_to[s]
        return (
            remote(meta_in.at[s, f], meta_in.at[to, f], s_meta.at[1], r_meta.at[to, f], place, 0, rep),
            remote(raw_in.at[s, f], raw_in.at[to, f], s_own.at[1], r_raw.at[to, f], place, 0, rep),
        )

    def row_copy(s, f, j):
        return remote(send_buf.at[s, f, j], rows.at[s, f, j], s_row, r_row.at[s], z, j, rep)

    def code_copy(s, f, j):
        src = meta_in.at[s, f, slot_count + xz_of[s]]
        return remote(src, codes.at[s, f, j], s_code, r_code.at[s], z, j, rep)

    def sq_copy(s):
        return remote(sq_own.at[s], sq_sib.at[s], s_sq, r_sq.at[s], z, 0, 1 - rep)

    def back_copy(s, f, j):
        to = back.at[(xz_of[s] * plane + j) * 2 + f]
        return remote(back_send.at[s, f], to, s_back, r_back, z_of[s], j, rep_of[f])

    def arrived(ref, sem):
        pltpu.make_async_copy(ref, ref, sem).wait()

    ref_copy = remote(refined_ref.at[:, mine], refined_ref.at[:, mine], s_ref, r_ref, z, 0, 1 - rep)
    ref_wait = remote(refined_ref.at[:, theirs], refined_ref.at[:, theirs], s_ref, r_ref, z, 0, 1 - rep)

    pl.semaphore_wait(barrier, plane + 2 + 2 * mid)
    local[0].wait()
    own_raw(1, 0).start()

    @pl.when(mid == 1)
    def _():
        own_raw(2, 0).start()

    local[1].wait()
    own_raw(0, 1).start()

    pltpu.make_async_copy(ints, ints, l_sem.at[2]).wait()
    raw_ids = ints[pl.ds(0, slot_count)]
    weights = ints[pl.ds(slot_count, slot_count)]
    table = ints[pl.ds(2 * slot_count, table_rows)]
    live = raw_ids >= 0
    safe_ids = jnp.maximum(raw_ids, 0)
    place = jnp.zeros((slot_count, row_count), jnp.int32)
    for r in range(table_rows):
        taken = take_lanes(table[r : r + 1], safe_ids % LANES)
        place = jnp.where(safe_ids // LANES == r, taken, place)
    owner = place // lists_here
    to_z, to_p = owner // plane, owner % plane

    def xor_two(a, b, bits):
        out = 0
        for i in range(bits):
            out = out + ((a // (1 << i) + b // (1 << i)) % 2) * (1 << i)
        return out

    turned = xor_two(to_z, z, 2) * plane + xor_two(to_p, p, pbits)
    turned = jnp.where(live, turned, -1)
    code = ((place % lists_here) * 8 + weights).astype(F32)
    square = (LANES, LANES)
    lane = iota(square, 1)
    sub = iota(square, 0)
    member = jnp.concatenate([(turned == o).astype(F32) for o in range(owners)], axis=0).astype(BF16)
    earlier = (sub < lane).astype(F32).astype(BF16)
    same_owner = sub // slot_count == lane // slot_count
    prior = (same_owner & (lane < sub)).astype(F32).astype(BF16)
    before = dot(prior, member).astype(BF16)
    rank_all = dot(member, earlier) + dot(before, jnp.ones(square, BF16))
    rank = jnp.zeros((slot_count, row_count), F32)
    for o in range(owners):
        rank = jnp.where(turned == o, rank_all[o * slot_count : (o + 1) * slot_count], rank)
    seat = jnp.where(live, turned.astype(F32) * cap + rank, -1.0)
    seat_keep[...] = seat
    for k in range(slot_count):
        meta_in[0, 0, k] = seat[k : k + 1]
    eye = sub == lane

    def to_row(col):
        return jnp.sum(jnp.where(eye, col, 0.0), axis=0, keepdims=True)

    def to_col(row):
        return jnp.sum(jnp.where(eye, row, 0.0), axis=1, keepdims=True)

    for g in range(LINE):
        q = (sub + g * LANES).astype(F32)
        found = jnp.zeros(square, F32)
        for k in range(slot_count):
            found = found + jnp.where(seat[k : k + 1] == q, code[k : k + 1], 0.0)
        meta_in[0, 0, slot_count + g] = to_row(jnp.sum(found, axis=1, keepdims=True))

    for f in range(2):
        own_meta(1, f).start()
    own_raw(1, 1).start()

    @pl.when(mid == 1)
    def _():
        for f in range(2):
            own_meta(2, f).start()
        own_raw(2, 1).start()

    own_meta(0, 1).start()

    def pick(s, f):
        if (s, f) != (0, 0):
            arrived(meta_in.at[s, f], r_meta.at[s, f])
        for j in range(1, plane):
            code_copy(s, f, j).start()
        if (s, f) != (0, 0):
            arrived(raw_in.at[s, f], r_raw.at[s, f])
        if s:

            @pl.when(mid == 1)
            def _():
                for copy in forward(s, f):
                    copy.start()

        q = (sub + xz_of[s] * LANES).astype(F32)
        chosen = jnp.zeros(square, F32)
        for k in range(slot_count):
            chosen = chosen + (meta_in[s, f, k] == q).astype(F32)
        picked = dot(chosen.astype(BF16), raw_in[s, f]).astype(BF16).reshape(plane, cap, half)
        send_buf[s, f] = picked
        for j in reversed(range(1, plane)):
            row_copy(s, f, j).start()
        rows[s, f, 0] = picked[0]

    lane_row = iota((1, LANES), 1)

    def code_row(s, f):
        out = meta_in[s, f, slot_count + xz_of[s]]
        for j in range(1, plane):
            out = jnp.where(lane_row // cap == j, codes[s, f, j], out)
        return out

    def halves(x):
        return x[:, :half] + x[:, half : 2 * half]

    def lane_parts(x):
        out = x[:, :LANES]
        for i in range(1, half // LANES):
            out = out + x[:, i * LANES : (i + 1) * LANES]
        return out

    def got_rows(s):
        return rows[s].reshape(2 * LANES, half).astype(F32)

    def near_part(s):
        arrived(codes.at[s, :, others], r_code.at[s])
        for f in range(2):
            row = code_row(s, f)
            wide = to_col(row).astype(jnp.int32) // 8
            masks[s, pl.ds(f * LANES, LANES)] = (
                (wide == iota((LANES, lists_here), 1)).astype(F32).astype(BF16)
            )
            placed[s, :, pl.ds(f * LANES, LANES)] = (
                (row.astype(jnp.int32) // 8 == iota((lists_here, LANES), 0)).astype(F32).astype(BF16)
            )
        centre = halves(dot(masks[s], cent_cat[...]))
        arrived(rows.at[s, :, others], r_row.at[s])
        diff = got_rows(s) - centre
        sq_own[s] = lane_parts(diff * diff)
        sq_copy(s).start()

    def far_part(s):
        weight = jnp.concatenate(
            [to_col((code_row(s, f).astype(jnp.int32) % 8).astype(F32)) for f in range(2)], axis=0
        )
        got = got_rows(s)
        sq_copy(s).wait_recv()
        swapped = jnp.concatenate([sq_sib[s, LANES:], sq_sib[s, :LANES]], axis=0)
        sq = jnp.sum(sq_own[s] + swapped, axis=1, keepdims=True)
        share = jnp.broadcast_to(weight / (1.0 + sq / (2 * half)), (2 * LANES, LANES))
        share_hi, share_lo = split_two(share)
        sv_hi, sv_lo = split_two(jnp.concatenate([share] * (half // LANES), axis=1) * got)
        added = dot(placed[s], jnp.concatenate([sv_hi, sv_lo, share_hi, share_lo], axis=1))
        sums = halves(added)
        counts = added[:, 2 * half : 2 * half + LANES] + added[:, 2 * half + LANES :]
        acc[...] = (cent[...] if s == 0 else acc[...]) + sums
        tot[...] = counts if s == 0 else tot[...] + counts

    pick(0, 0)
    local[5].wait()
    hi, lo = split_two(cent[...])
    cent_cat[:, pl.ds(0, half)] = hi
    cent_cat[:, pl.ds(half, half)] = lo
    pick(0, 1)

    def follow(steps):
        for step, args in steps:
            step(*args)

    @pl.when(mid == 1)
    def _():
        follow([
            (pick, (2, 0)), (pick, (1, 0)), (pick, (2, 1)), (pick, (1, 1)), (near_part, (0,)), (pick, (3, 0)), (pick, (3, 1)),
            (far_part, (0,)), (near_part, (1,)), (near_part, (2,)), (far_part, (1,)), (near_part, (3,)), (far_part, (2,)),
            (far_part, (3,)),
        ])

    @pl.when(mid == 0)
    def _():
        follow([
            (pick, (1, 0)), (pick, (1, 1)), (near_part, (0,)), (pick, (2, 0)), (near_part, (1,)), (far_part, (0,)), (pick, (2, 1)),
            (far_part, (1,)), (pick, (3, 0)), (near_part, (2,)), (pick, (3, 1)), (near_part, (3,)), (far_part, (2,)),
            (far_part, (3,)),
        ])

    scale = 1.0 / (1.0 + tot[...])
    refined = acc[...] * jnp.concatenate([scale] * (half // LANES), axis=1)
    refined_ref[:, mine] = refined
    hi, lo = split_two(refined)
    cent_cat[:, pl.ds(0, half)] = hi
    cent_cat[:, pl.ds(half, half)] = lo

    for s in reversed(range(LINE)):
        diff = got_rows(s) - halves(dot(masks[s], cent_cat[...]))
        value = jnp.sum(lane_parts(diff * diff), axis=1, keepdims=True) / (2 * half)
        for f in range(2):
            row = to_row(value[f * LANES : (f + 1) * LANES])
            back_send[s, f] = row
            for j in range(plane):
                if (s, f, j) != (0, 0, 0):
                    back_copy(s, f, j).start()
            if (s, f) == (0, 0):
                back[0] = row
        if s == 2:
            ref_copy.start()

    seats = seat_keep[...].astype(jnp.int32)
    lanes_at = jnp.maximum(seats, 0) % LANES
    out = jnp.zeros((slot_count, row_count), F32)
    arrived(back.at[pl.ds(1, 2 * owners - 1)], r_back)
    for x in range(LINE):
        line = jnp.zeros((1, LANES), F32)
        for j in range(plane):
            first = (x * plane + j) * 2
            line = jnp.where(lane_row // cap == j, back[first] + back[first + 1], line)
        taken = take_lanes(line, lanes_at)
        out = jnp.where((seats >= 0) & (seats // LANES == x), taken, out)
    dist_ref[...] = out

    ref_wait.wait_recv()
    ref_copy.wait_send()
    arrived(raw_in.at[pl.ds(0, 3), 0], s_own.at[0])
    arrived(meta_in.at[pl.ds(0, 3), 0], s_meta.at[0])

    @pl.when(mid == 1)
    def _():
        arrived(raw_in, s_own.at[1])
        arrived(meta_in, s_meta.at[1])

    arrived(sq_own, s_sq)
    arrived(rows.at[:, :, others], s_row)
    arrived(codes.at[:, :, others], s_code)
    arrived(back.at[pl.ds(1, 2 * owners - 1)], s_back)


def shards(vectors, list_ids, spill_weight, list_pos, old_centroids):
    owners = lax.axis_size("grp")
    row_count, slot_count = list_ids.shape
    feature_dim = vectors.shape[1]
    lists_here = old_centroids.shape[0]
    cap = row_count * slot_count // (2 * owners)
    plane = owners // LINE
    fits = (
        row_count == LANES and slot_count == 8 and owners * cap == LINE * LANES and plane & (plane - 1) == 0
        and owners * slot_count == LANES and cap % 16 == 0 and lax.axis_size("rep") == 2
        and lists_here % LANES == 0 and feature_dim % (2 * LANES) == 0 and list_pos.shape[0] % LANES == 0
    )
    if not fits:
        return shards_general(vectors, list_ids, spill_weight, list_pos, old_centroids)
    half = feature_dim // 2
    table_rows = list_pos.shape[0] // LANES
    meta_rows = slot_count + LINE
    vmem = pl.BlockSpec(memory_space=pltpu.VMEM)
    hbm = pl.BlockSpec(memory_space=pl.ANY)
    dma = pltpu.SemaphoreType.DMA
    refined, dist = pl.pallas_call(
        functools.partial(line_kernel, owners, cap),
        out_shape=(
            pltpu.VMEM((lists_here, feature_dim), F32),
            pltpu.VMEM((slot_count, row_count), F32),
        ),
        in_specs=[hbm] * 5,
        out_specs=(vmem, vmem),
        scratch_shapes=[
            pltpu.VMEM((2 * slot_count + table_rows, LANES), jnp.int32),
            pltpu.VMEM((row_count, half), BF16),
            pltpu.VMEM((lists_here, half), F32),
            pltpu.VMEM((lists_here, feature_dim), BF16),
            pltpu.VMEM((LINE, 2, row_count, half), BF16),
            pltpu.VMEM((LINE, 2, meta_rows, 1, LANES), F32),
            pltpu.VMEM((slot_count, row_count), F32),
            pltpu.VMEM((LINE, 2, plane, cap, half), BF16),
            pltpu.VMEM((LINE, 2, plane, cap, half), BF16),
            pltpu.VMEM((LINE, 2, plane, 1, LANES), F32),
            pltpu.VMEM((LINE, 2 * LANES, lists_here), BF16),
            pltpu.VMEM((LINE, lists_here, 2 * LANES), BF16),
            pltpu.VMEM((LINE, 2 * LANES, LANES), F32),
            pltpu.VMEM((LINE, 2 * LANES, LANES), F32),
            pltpu.VMEM((lists_here, half), F32),
            pltpu.VMEM((lists_here, LANES), F32),
            pltpu.VMEM((LINE, 2, 1, LANES), F32),
            pltpu.VMEM((2 * owners, 1, LANES), F32),
            dma((4,)),
            dma((2,)), dma((2,)), dma((LINE, 2)), dma((LINE, 2)),
            dma(()), dma((LINE,)), dma(()), dma((LINE,)), dma(()), dma((LINE,)),
            dma(()), dma(()), dma(()), dma(()),
        ],
        compiler_params=pltpu.CompilerParams(collective_id=0, has_side_effects=True),
    )(vectors, list_ids.T, spill_weight.T, list_pos.reshape(-1, LANES), old_centroids)
    return refined, dist.T


def solution(mesh):
    return jax.shard_map(
        shards,
        mesh=mesh,
        in_specs=(
            P(("grp", "rep"), None),
            P(("grp", "rep"), None),
            P(("grp", "rep"), None),
            P(),
            P("grp", None),
        ),
        out_specs=(P("grp", None), P(("grp", "rep"), None)),
        check_vma=False,
    )
```

```python
import functools
import math

import jax
import jax.numpy as jnp
from jax import lax
from jax.experimental import pallas as pl
from jax.experimental.pallas import tpu as pltpu
from jax.sharding import PartitionSpec as P

D = 768


def decode_meta(meta_rows):
    values = meta_rows.astype(jnp.int32)
    tag_value = values[:, 0] * 128 + values[:, 1]
    return (tag_value > 0, jnp.maximum(tag_value - 1, 0), values[:, 2].astype(jnp.float32))


def pick_block(table, index_block):
    table_iota = jnp.arange(table.shape[0], dtype=jnp.int32)
    if table.dtype == jnp.float32:
        selector = (index_block[:, None] == table_iota[None, :]).astype(jnp.float32)
        return jnp.dot(
            selector, table, precision=lax.Precision.HIGHEST, preferred_element_type=jnp.float32
        )
    selector = (index_block[:, None] == table_iota[None, :]).astype(table.dtype)
    return jnp.dot(selector, table, preferred_element_type=jnp.float32).astype(table.dtype)


def pick_rows(table, indices):
    total_rows = indices.shape[0]
    block_rows = math.gcd(512, total_rows)
    block_count = total_rows // block_rows
    picked = lax.map(
        lambda index_block: pick_block(table, index_block), indices.reshape(block_count, block_rows)
    )
    return picked.reshape(total_rows, table.shape[1])


def owner_sums(rows_all, slot_all, weight_all, old_centroids, lists_here):
    total_rows, feature_dim = rows_all.shape
    block_rows = math.gcd(512, total_rows)
    block_count = total_rows // block_rows
    row_blocks = rows_all.reshape(block_count, block_rows, feature_dim)
    slot_blocks = slot_all.reshape(block_count, block_rows)
    weight_blocks = weight_all.reshape(block_count, block_rows)
    list_iota = jnp.arange(lists_here, dtype=jnp.int32)

    def accumulate(running, piece_item):
        weighted_sums, totals = running
        rows_in, slot_in, weight_in = piece_item
        row_values = rows_in.astype(jnp.float32)
        centre_rows = pick_block(old_centroids, slot_in)
        sq_norms = jnp.sum((row_values - centre_rows) ** 2, axis=-1)
        shares = weight_in / (1.0 + sq_norms / D)
        placed = (slot_in[None, :] == list_iota[:, None]).astype(jnp.float32) * shares[None, :]
        weighted_sums = weighted_sums + jnp.dot(
            placed, row_values, precision=lax.Precision.HIGHEST, preferred_element_type=jnp.float32
        )
        totals = totals + jnp.sum(placed, axis=1)
        return ((weighted_sums, totals), jnp.float32(0.0))

    start_state = (
        jnp.zeros((lists_here, feature_dim), jnp.float32),
        jnp.zeros((lists_here,), jnp.float32),
    )
    final_state, unused = lax.scan(
        accumulate, start_state, (row_blocks, slot_blocks, weight_blocks)
    )
    return final_state


def shards_general(vectors, list_ids, spill_weight, list_pos, old_centroids):
    owners = lax.axis_size("grp")
    row_count, slot_count = list_ids.shape
    feature_dim = vectors.shape[1]
    lists_here = old_centroids.shape[0]
    cap_slots = row_count * slot_count // (2 * owners)
    seat_total = owners * cap_slots
    pair_count = row_count * slot_count
    is_live = list_ids >= 0
    places = jnp.where(is_live, list_pos[jnp.maximum(list_ids, 0)], 0)
    target = jnp.where(is_live, places // lists_here, owners).reshape(-1)
    sorted_order = jnp.argsort(target, stable=True)
    ranked = target[sorted_order]
    counts = jnp.sum(
        (target[:, None] == jnp.arange(owners, dtype=jnp.int32)[None, :]).astype(jnp.int32), axis=0
    )
    starts = jnp.concatenate([jnp.cumsum(counts) - counts, jnp.zeros((1,), jnp.int32)])
    within = jnp.arange(pair_count, dtype=jnp.int32) - starts[ranked]
    seat_sorted = jnp.where(ranked < owners, ranked * cap_slots + within, seat_total)
    seat_index = jnp.zeros((pair_count,), jnp.int32).at[sorted_order].set(seat_sorted)
    pair_of_seat = (
        jnp.full((seat_total,), -1, jnp.int32)
        .at[seat_index]
        .set(jnp.arange(pair_count, dtype=jnp.int32), mode="drop")
    )
    filled = pair_of_seat >= 0
    pair_safe = jnp.maximum(pair_of_seat, 0)
    source_row = jnp.where(filled, pair_safe // slot_count, -1)
    send_rows = pick_rows(vectors, source_row)
    local_flat = (places % lists_here).reshape(-1)
    weight_flat = spill_weight.reshape(-1)
    tag_out = jnp.where(filled, local_flat[pair_safe] + 1, 0)
    weight_out = jnp.where(filled, weight_flat[pair_safe], 0)
    send_meta = jnp.stack([tag_out // 128, tag_out % 128, weight_out], axis=-1).astype(jnp.bfloat16)
    got_rows, got_meta = (
        lax.all_to_all(
            send_rows.reshape(owners, cap_slots, feature_dim),
            "grp",
            split_axis=0,
            concat_axis=0,
            tiled=True,
        ),
        lax.all_to_all(
            send_meta.reshape(owners, cap_slots, 3), "grp", split_axis=0, concat_axis=0, tiled=True
        ),
    )
    got_rows = got_rows.reshape(seat_total, feature_dim)
    got_meta = got_meta.reshape(seat_total, 3)
    seat_live, seat_row, seat_weight = decode_meta(got_meta)
    weighted_sums, totals = owner_sums(got_rows, seat_row, seat_weight, old_centroids, lists_here)
    weighted_sums, totals = lax.psum((weighted_sums, totals), "rep")
    refined = (old_centroids + weighted_sums) / (1.0 + totals[:, None])
    block_rows = math.gcd(512, seat_total)
    block_count = seat_total // block_rows
    row_blocks = got_rows.reshape(block_count, block_rows, feature_dim)
    slot_blocks = seat_row.reshape(block_count, block_rows)

    def distance(piece_item):
        rows_in, slot_in = piece_item
        row_values = rows_in.astype(jnp.float32)
        return jnp.sum((row_values - pick_block(refined, slot_in)) ** 2, axis=-1) / D

    owner_dist = lax.map(distance, (row_blocks, slot_blocks)).reshape(owners, cap_slots)
    seat_dist = lax.all_to_all(owner_dist, "grp", split_axis=0, concat_axis=0, tiled=True).reshape(
        seat_total
    )
    picked = seat_dist[jnp.minimum(seat_index, seat_total - 1)].reshape(row_count, slot_count)
    new_dist = jnp.where(is_live, picked, jnp.float32(0.0))
    return (refined, new_dist)


MESH = pl.DeviceIdType.MESH
LANES = 128
LINE = 4
F32 = jnp.float32
BF16 = jnp.bfloat16


def xor_index(a, b_const, bits):
    out = 0
    for i in range(bits):
        bit = (a // (1 << i)) % 2
        out = out + ((1 - bit) if (b_const >> i) & 1 else bit) * (1 << i)
    return out


def split_two(x):
    hi = x.astype(BF16)
    return hi, (x - hi.astype(F32)).astype(BF16)


def dot(a, b):
    return jnp.dot(a, b, preferred_element_type=F32)


def iota(shape, dim):
    return lax.broadcasted_iota(jnp.int32, shape, dim)


def take_lanes(line, at):
    wide = jnp.broadcast_to(line, at.shape)
    return jnp.take_along_axis(wide, at, axis=1, mode="promise_in_bounds")


def line_kernel(
    owners, cap,
    vec_hbm, ids_hbm, weight_hbm, pos_hbm, cent_hbm,
    refined_ref, dist_ref,
    ints, vec_other, cent, cent_cat, raw_in, meta_in, seat_keep, send_buf, send_near, rows, codes,
    masks, placed, sq_own, sq_sib, acc, tot, back_send, back,
    l_sem, s_own, s_meta, r_raw, r_meta, s_row, r_row, s_code, r_code, s_sq, r_sq, s_back, r_back, s_ref, r_ref, s_near, first, second,
):
    me = lax.axis_index("grp")
    rep = lax.axis_index("rep")
    slot_count, row_count = seat_keep.shape
    lists_here, half = cent.shape
    table_rows = pos_hbm.shape[0]
    plane = owners // LINE
    pbits = plane.bit_length() - 1
    z = me // plane
    p = me % plane
    mid = ((z + 1) // 2) % 2
    near = z + 1 - 2 * (z % 2)
    inner = LINE - 1 - z
    cross = (z + 2) % LINE
    z_of = [z, near, mid * inner + (1 - mid) * cross, mid * cross + (1 - mid) * inner]
    xz_of = [0, 1, 2 + mid, 3 - mid]
    rep_of = [rep, 1 - rep]
    mine = pl.ds(pl.multiple_of(rep * half, LANES), half)
    theirs = pl.ds(pl.multiple_of((1 - rep) * half, LANES), half)

    def at(place, xp):
        return place * plane + xor_index(p, xp, pbits)

    barrier = pltpu.get_barrier_semaphore()

    def greet(place, xp, r):
        pl.semaphore_signal(barrier, inc=1, device_id={"grp": at(place, xp), "rep": r}, device_id_type=MESH)

    greet(near, 0, 0)
    greet(near, 0, 1)

    @pl.when(mid == 1)
    def _():
        greet(inner, 0, 0)
        greet(inner, 0, 1)

    for i in range(pbits):
        greet(z, 1 << i, rep)
    greet(z, 0, 1 - rep)

    local = [
        pltpu.make_async_copy(vec_hbm.at[:, mine], raw_in.at[0, 0], l_sem.at[0]),
        pltpu.make_async_copy(vec_hbm.at[:, theirs], vec_other, l_sem.at[1]),
        pltpu.make_async_copy(ids_hbm, ints.at[pl.ds(0, slot_count)], l_sem.at[2]),
        pltpu.make_async_copy(weight_hbm, ints.at[pl.ds(slot_count, slot_count)], l_sem.at[2]),
        pltpu.make_async_copy(pos_hbm, ints.at[pl.ds(2 * slot_count, table_rows)], l_sem.at[2]),
        pltpu.make_async_copy(cent_hbm.at[:, mine], cent, l_sem.at[3]),
    ]
    for copy in local:
        copy.start()

    def tell(semaphore, steps):
        for j in steps:
            pl.semaphore_signal(semaphore, inc=1, device_id={"grp": at(z, j), "rep": rep}, device_id_type=MESH)

    def remote(src, dst, send, recv, place, xp, r):
        return pltpu.make_async_remote_copy(
            src_ref=src, dst_ref=dst, send_sem=send, recv_sem=recv,
            device_id={"grp": at(place, xp), "rep": r}, device_id_type=MESH,
        )

    own_place = [z, near, inner]
    others = pl.ds(1, plane - 1)

    def own_raw(s, f):
        src = raw_in.at[0, 0] if f == 0 else vec_other
        return remote(src, raw_in.at[s, f], s_own.at[s // 2], r_raw.at[s, f], own_place[s], 0, rep_of[f])

    def own_meta(s, f):
        return remote(
            meta_in.at[0, 0], meta_in.at[s, f], s_meta.at[s // 2], r_meta.at[s, f], own_place[s], 0, rep_of[f]
        )

    def forward(f):
        return (
            remote(meta_in.at[1, f], meta_in.at[3, f], s_meta.at[1], r_meta.at[3, f], inner, 0, rep),
            remote(raw_in.at[1, f], raw_in.at[3, f], s_own.at[1], r_raw.at[3, f], inner, 0, rep),
        )

    def row_copy(s, f, j):
        return remote(send_buf.at[s, f, j], rows.at[s, f, j], s_row, r_row.at[s], z, j, rep)

    def code_copy(s, f, j):
        src = meta_in.at[s, f, slot_count + xz_of[s]]
        return remote(src, codes.at[s, f, j], s_code, r_code.at[s], z, j, rep)

    def near_row_copy(s, f, j):
        return remote(send_near.at[s - 2, f, j], rows.at[s, f, j], s_own.at[1], r_row.at[s], near, j, rep)

    def near_code_copy(s, f, j):
        src = meta_in.at[s, f, slot_count + s]
        return remote(src, codes.at[s, f, j], s_near, r_code.at[s], near, j, rep)

    def sq_copy(s):
        return remote(sq_own.at[s], sq_sib.at[s], s_sq, r_sq.at[s], z, 0, 1 - rep)

    def back_copy(s, f, j):
        to = back.at[(xz_of[s] * plane + j) * 2 + f]
        return remote(back_send.at[s, f], to, s_back, r_back, z_of[s], j, rep_of[f])

    def arrived(ref, sem):
        pltpu.make_async_copy(ref, ref, sem).wait()

    ref_copy = remote(refined_ref.at[:, mine], refined_ref.at[:, mine], s_ref, r_ref, z, 0, 1 - rep)
    ref_wait = remote(refined_ref.at[:, theirs], refined_ref.at[:, theirs], s_ref, r_ref, z, 0, 1 - rep)

    pl.semaphore_wait(barrier, pbits + 3 + 2 * mid)
    def own_to(f):
        own_raw(1, f).start()

        @pl.when(mid == 1)
        def _():
            own_raw(2, f).start()

    tell(first, [1 << i for i in range(pbits)])
    local[0].wait()
    own_to(0)
    local[1].wait()
    own_raw(0, 1).start()
    pltpu.make_async_copy(ints, ints, l_sem.at[2]).wait()
    raw_ids = ints[pl.ds(0, slot_count)]
    weights = ints[pl.ds(slot_count, slot_count)]
    table = ints[pl.ds(2 * slot_count, table_rows)]
    live = raw_ids >= 0
    safe_ids = jnp.maximum(raw_ids, 0)
    place = jnp.zeros((slot_count, row_count), jnp.int32)
    for r in range(table_rows):
        taken = take_lanes(table[r : r + 1], safe_ids % LANES)
        place = jnp.where(safe_ids // LANES == r, taken, place)
    owner = place // lists_here
    to_z, to_p = owner // plane, owner % plane

    def xor_two(a, b, bits):
        out = 0
        for i in range(bits):
            out = out + ((a // (1 << i) + b // (1 << i)) % 2) * (1 << i)
        return out

    turned = xor_two(to_z, z, 2) * plane + xor_two(to_p, p, pbits)
    turned = jnp.where(live, turned, -1)
    code = ((place % lists_here) * 8 + weights).astype(F32)
    square = (LANES, LANES)
    lane = iota(square, 1)
    sub = iota(square, 0)
    member = jnp.concatenate([(turned == o).astype(F32) for o in range(owners)], axis=0).astype(BF16)
    earlier = (sub < lane).astype(F32).astype(BF16)
    same_owner = sub // slot_count == lane // slot_count
    prior = (same_owner & (lane < sub)).astype(F32).astype(BF16)
    before = dot(prior, member).astype(BF16)
    rank_all = dot(member, earlier) + dot(before, jnp.ones(square, BF16))
    rank = jnp.zeros((slot_count, row_count), F32)
    for o in range(owners):
        rank = jnp.where(turned == o, rank_all[o * slot_count : (o + 1) * slot_count], rank)
    seat = jnp.where(live, turned.astype(F32) * cap + rank, -1.0)
    seat_keep[...] = seat
    for k in range(slot_count):
        meta_in[0, 0, k] = seat[k : k + 1]
    eye = sub == lane

    def to_row(col):
        return jnp.sum(jnp.where(eye, col, 0.0), axis=0, keepdims=True)

    def to_col(row):
        return jnp.sum(jnp.where(eye, row, 0.0), axis=1, keepdims=True)

    for g in range(LINE):
        q = (sub + g * LANES).astype(F32)
        found = jnp.zeros(square, F32)
        for k in range(slot_count):
            found = found + jnp.where(seat[k : k + 1] == q, code[k : k + 1], 0.0)
        meta_in[0, 0, slot_count + g] = to_row(jnp.sum(found, axis=1, keepdims=True))

    for f in range(2):
        own_meta(1, f).start()

    @pl.when(mid == 1)
    def _():
        for f in range(2):
            own_meta(2, f).start()

    own_to(1)
    own_meta(0, 1).start()

    def picked_rows(s, f, xz):
        q = (sub + xz * LANES).astype(F32)
        chosen = jnp.zeros(square, F32)
        for k in range(slot_count):
            chosen = chosen + (meta_in[s, f, k] == q).astype(F32)
        return dot(chosen.astype(BF16), raw_in[s, f]).astype(BF16).reshape(plane, cap, half)

    def pick(s, f):
        to_near = s >= 2
        if (s, f) != (0, 0):
            arrived(meta_in.at[s, f], r_meta.at[s, f])
        for j in reversed(range(plane)):
            if to_near:
                near_code_copy(s, f, j).start()
            if j and (s, f) != (0, 0):
                code_copy(s, f, j).start()
        if (s, f) != (0, 0):
            arrived(raw_in.at[s, f], r_raw.at[s, f])
        if to_near:
            send_near[s - 2, f] = picked_rows(s, f, s)
            for j in reversed(range(plane)):
                near_row_copy(s, f, j).start()
        elif s:

            @pl.when(mid == 1)
            def _():
                for copy in forward(f):
                    copy.start()

        picked = picked_rows(s, f, xz_of[s])
        send_buf[s, f] = picked
        if (s, f) == (0, 0):
            pl.semaphore_wait(first, pbits)
            tell(second, [1])
            for j in reversed(range(1, plane)):
                code_copy(s, f, j).start()
        for j in reversed(range(1, plane)):
            row_copy(s, f, j).start()
        rows[s, f, 0] = picked[0]

    lane_row = iota((1, LANES), 1)

    def code_row(s, f, picked_here=True):
        out = meta_in[s, f, slot_count + xz_of[s]] if picked_here else codes[s, f, 0]
        for j in range(1, plane):
            out = jnp.where(lane_row // cap == j, codes[s, f, j], out)
        return out

    def halves(x):
        return x[:, :half] + x[:, half : 2 * half]

    def lane_parts(x):
        out = x[:, :LANES]
        for i in range(1, half // LANES):
            out = out + x[:, i * LANES : (i + 1) * LANES]
        return out

    def got_rows(s):
        return rows[s].reshape(2 * LANES, half).astype(F32)

    def near_part(s, picked_here=True):
        arrived(codes.at[s, :, others] if picked_here else codes.at[s], r_code.at[s])
        for f in range(2):
            row = code_row(s, f, picked_here)
            wide = to_col(row).astype(jnp.int32) // 8
            masks[s, pl.ds(f * LANES, LANES)] = (
                (wide == iota((LANES, lists_here), 1)).astype(F32).astype(BF16)
            )
            placed[s, :, pl.ds(f * LANES, LANES)] = (
                (row.astype(jnp.int32) // 8 == iota((lists_here, LANES), 0)).astype(F32).astype(BF16)
            )
        centre = halves(dot(masks[s], cent_cat[...]))
        arrived(rows.at[s, :, others] if picked_here else rows.at[s], r_row.at[s])
        diff = got_rows(s) - centre
        sq_own[s] = lane_parts(diff * diff)
        sq_copy(s).start()

    def far_part(s, picked_here=True):
        weight = jnp.concatenate(
            [to_col((code_row(s, f, picked_here).astype(jnp.int32) % 8).astype(F32)) for f in range(2)], axis=0
        )
        got = got_rows(s)
        sq_copy(s).wait_recv()
        swapped = jnp.concatenate([sq_sib[s, LANES:], sq_sib[s, :LANES]], axis=0)
        sq = jnp.sum(sq_own[s] + swapped, axis=1, keepdims=True)
        share = jnp.broadcast_to(weight / (1.0 + sq / (2 * half)), (2 * LANES, LANES))
        share_hi, share_lo = split_two(share)
        sv_hi, sv_lo = split_two(jnp.concatenate([share] * (half // LANES), axis=1) * got)
        added = dot(placed[s], jnp.concatenate([sv_hi, sv_lo, share_hi, share_lo], axis=1))
        sums = halves(added)
        counts = added[:, 2 * half : 2 * half + LANES] + added[:, 2 * half + LANES :]
        acc[...] = (cent[...] if s == 0 else acc[...]) + sums
        tot[...] = counts if s == 0 else tot[...] + counts

    pick(0, 0)
    local[5].wait()
    hi, lo = split_two(cent[...])
    cent_cat[:, pl.ds(0, half)] = hi
    cent_cat[:, pl.ds(half, half)] = lo
    pick(0, 1)

    def follow(steps):
        for step, args in steps:
            step(*args)

    @pl.when(mid == 1)
    def _():
        pl.semaphore_wait(second, 1)
        follow([
            (pick, (1, 0)), (pick, (2, 0)), (pick, (1, 1)), (pick, (2, 1)), (near_part, (0,)), (pick, (3, 0)), (pick, (3, 1)),
            (far_part, (0,)), (near_part, (1,)), (near_part, (2,)), (far_part, (1,)), (near_part, (3,)), (far_part, (2,)),
            (far_part, (3,)),
        ])

    @pl.when(mid == 0)
    def _():
        pl.semaphore_wait(second, 1)
        follow([
            (pick, (1, 0)), (pick, (1, 1)), (near_part, (0,)), (near_part, (1,)), (far_part, (0,)), (far_part, (1,)),
            (near_part, (2, False)), (near_part, (3, False)), (far_part, (2, False)), (far_part, (3, False)),
        ])

    scale = 1.0 / (1.0 + tot[...])
    refined = acc[...] * jnp.concatenate([scale] * (half // LANES), axis=1)
    refined_ref[:, mine] = refined
    hi, lo = split_two(refined)
    cent_cat[:, pl.ds(0, half)] = hi
    cent_cat[:, pl.ds(half, half)] = lo

    for s in reversed(range(LINE)):
        diff = got_rows(s) - halves(dot(masks[s], cent_cat[...]))
        value = jnp.sum(lane_parts(diff * diff), axis=1, keepdims=True) / (2 * half)
        for f in range(2):
            row = to_row(value[f * LANES : (f + 1) * LANES])
            back_send[s, f] = row
            for j in range(plane):
                if (s, f, j) != (0, 0, 0):
                    back_copy(s, f, j).start()
            if (s, f) == (0, 0):
                back[0] = row
        if s == 2:
            ref_copy.start()

    seats = seat_keep[...].astype(jnp.int32)
    lanes_at = jnp.maximum(seats, 0) % LANES
    out = jnp.zeros((slot_count, row_count), F32)
    arrived(back.at[pl.ds(1, 2 * owners - 1)], r_back)
    for x in range(LINE):
        line = jnp.zeros((1, LANES), F32)
        for j in range(plane):
            first = (x * plane + j) * 2
            line = jnp.where(lane_row // cap == j, back[first] + back[first + 1], line)
        taken = take_lanes(line, lanes_at)
        out = jnp.where((seats >= 0) & (seats // LANES == x), taken, out)
    dist_ref[...] = out

    ref_wait.wait_recv()
    ref_copy.wait_send()
    arrived(raw_in.at[pl.ds(0, 3), 0], s_own.at[0])
    arrived(meta_in.at[pl.ds(0, 3), 0], s_meta.at[0])

    @pl.when(mid == 1)
    def _():
        arrived(raw_in, s_own.at[1])
        arrived(meta_in.at[pl.ds(0, 2)], s_meta.at[1])
        arrived(rows.at[:, :, others], s_row)
        arrived(codes.at[:, :, others], s_code)
        arrived(codes.at[pl.ds(2, 2)], s_near)

    @pl.when(mid == 0)
    def _():
        arrived(rows.at[pl.ds(0, 2), :, others], s_row)
        arrived(codes.at[pl.ds(0, 2), :, others], s_code)

    arrived(sq_own, s_sq)
    arrived(back.at[pl.ds(1, 2 * owners - 1)], s_back)


def store_kernel(refined_ref, dist_ref, refined_out, dist_out, refined_sem, dist_sem):
    copies = [
        pltpu.make_async_copy(refined_ref, refined_out, refined_sem),
        pltpu.make_async_copy(dist_ref, dist_out, dist_sem),
    ]
    for copy in copies:
        copy.start()
    for copy in copies:
        copy.wait()


def shards(vectors, list_ids, spill_weight, list_pos, old_centroids):
    owners = lax.axis_size("grp")
    row_count, slot_count = list_ids.shape
    feature_dim = vectors.shape[1]
    lists_here = old_centroids.shape[0]
    cap = row_count * slot_count // (2 * owners)
    plane = owners // LINE
    fits = (
        row_count == LANES and slot_count == 8 and owners * cap == LINE * LANES and plane == 4
        and owners * slot_count == LANES and cap % 16 == 0 and lax.axis_size("rep") == 2
        and lists_here % LANES == 0 and feature_dim % (2 * LANES) == 0 and list_pos.shape[0] % LANES == 0
    )
    if not fits:
        return shards_general(vectors, list_ids, spill_weight, list_pos, old_centroids)
    half = feature_dim // 2
    table_rows = list_pos.shape[0] // LANES
    meta_rows = slot_count + LINE
    vmem = pl.BlockSpec(memory_space=pltpu.VMEM)
    hbm = pl.BlockSpec(memory_space=pl.ANY)
    dma = pltpu.SemaphoreType.DMA
    refined, dist = pl.pallas_call(
        functools.partial(line_kernel, owners, cap),
        out_shape=(
            pltpu.VMEM((lists_here, feature_dim), F32),
            pltpu.VMEM((slot_count, row_count), F32),
        ),
        in_specs=[hbm] * 5,
        out_specs=(vmem, vmem),
        scratch_shapes=[
            pltpu.VMEM((2 * slot_count + table_rows, LANES), jnp.int32),
            pltpu.VMEM((row_count, half), BF16),
            pltpu.VMEM((lists_here, half), F32),
            pltpu.VMEM((lists_here, feature_dim), BF16),
            pltpu.VMEM((LINE, 2, row_count, half), BF16),
            pltpu.VMEM((LINE, 2, meta_rows, 1, LANES), F32),
            pltpu.VMEM((slot_count, row_count), F32),
            pltpu.VMEM((LINE, 2, plane, cap, half), BF16),
            pltpu.VMEM((2, 2, plane, cap, half), BF16),
            pltpu.VMEM((LINE, 2, plane, cap, half), BF16),
            pltpu.VMEM((LINE, 2, plane, 1, LANES), F32),
            pltpu.VMEM((LINE, 2 * LANES, lists_here), BF16),
            pltpu.VMEM((LINE, lists_here, 2 * LANES), BF16),
            pltpu.VMEM((LINE, 2 * LANES, LANES), F32),
            pltpu.VMEM((LINE, 2 * LANES, LANES), F32),
            pltpu.VMEM((lists_here, half), F32),
            pltpu.VMEM((lists_here, LANES), F32),
            pltpu.VMEM((LINE, 2, 1, LANES), F32),
            pltpu.VMEM((2 * owners, 1, LANES), F32),
            dma((4,)),
            dma((2,)), dma((2,)), dma((LINE, 2)), dma((LINE, 2)),
            dma(()), dma((LINE,)), dma(()), dma((LINE,)), dma(()), dma((LINE,)),
            dma(()), dma(()), dma(()), dma(()), dma(()), pltpu.SemaphoreType.REGULAR,
            pltpu.SemaphoreType.REGULAR,
        ],
        compiler_params=pltpu.CompilerParams(collective_id=0, has_side_effects=True),
    )(vectors, list_ids.T, spill_weight.T, list_pos.reshape(-1, LANES), old_centroids)
    refined, dist = pl.pallas_call(
        store_kernel,
        out_shape=(
            pltpu.HBM((lists_here, feature_dim), F32),
            pltpu.HBM((slot_count, row_count), F32),
        ),
        in_specs=[vmem, vmem],
        out_specs=(hbm, hbm),
        scratch_shapes=[dma(()), dma(())],
    )(*(pltpu.with_memory_space_constraint(x, pltpu.MemorySpace.VMEM) for x in (refined, dist)))
    return refined, dist.T


def solution(mesh):
    return jax.shard_map(
        shards,
        mesh=mesh,
        in_specs=(
            P(("grp", "rep"), None),
            P(("grp", "rep"), None),
            P(("grp", "rep"), None),
            P(),
            P("grp", None),
        ),
        out_specs=(P("grp", None), P(("grp", "rep"), None)),
        check_vma=False,
    )
```

```python
import functools
import math

import jax
import jax.numpy as jnp
from jax import lax
from jax.experimental import pallas as pl
from jax.experimental.pallas import tpu as pltpu
from jax.sharding import PartitionSpec as P

D = 768


def decode_meta(meta_rows):
    values = meta_rows.astype(jnp.int32)
    tag_value = values[:, 0] * 128 + values[:, 1]
    return (tag_value > 0, jnp.maximum(tag_value - 1, 0), values[:, 2].astype(jnp.float32))


def pick_block(table, index_block):
    table_iota = jnp.arange(table.shape[0], dtype=jnp.int32)
    if table.dtype == jnp.float32:
        selector = (index_block[:, None] == table_iota[None, :]).astype(jnp.float32)
        return jnp.dot(
            selector, table, precision=lax.Precision.HIGHEST, preferred_element_type=jnp.float32
        )
    selector = (index_block[:, None] == table_iota[None, :]).astype(table.dtype)
    return jnp.dot(selector, table, preferred_element_type=jnp.float32).astype(table.dtype)


def pick_rows(table, indices):
    total_rows = indices.shape[0]
    block_rows = math.gcd(512, total_rows)
    block_count = total_rows // block_rows
    picked = lax.map(
        lambda index_block: pick_block(table, index_block), indices.reshape(block_count, block_rows)
    )
    return picked.reshape(total_rows, table.shape[1])


def owner_sums(rows_all, slot_all, weight_all, old_centroids, lists_here):
    total_rows, feature_dim = rows_all.shape
    block_rows = math.gcd(512, total_rows)
    block_count = total_rows // block_rows
    row_blocks = rows_all.reshape(block_count, block_rows, feature_dim)
    slot_blocks = slot_all.reshape(block_count, block_rows)
    weight_blocks = weight_all.reshape(block_count, block_rows)
    list_iota = jnp.arange(lists_here, dtype=jnp.int32)

    def accumulate(running, piece_item):
        weighted_sums, totals = running
        rows_in, slot_in, weight_in = piece_item
        row_values = rows_in.astype(jnp.float32)
        centre_rows = pick_block(old_centroids, slot_in)
        sq_norms = jnp.sum((row_values - centre_rows) ** 2, axis=-1)
        shares = weight_in / (1.0 + sq_norms / D)
        placed = (slot_in[None, :] == list_iota[:, None]).astype(jnp.float32) * shares[None, :]
        weighted_sums = weighted_sums + jnp.dot(
            placed, row_values, precision=lax.Precision.HIGHEST, preferred_element_type=jnp.float32
        )
        totals = totals + jnp.sum(placed, axis=1)
        return ((weighted_sums, totals), jnp.float32(0.0))

    start_state = (
        jnp.zeros((lists_here, feature_dim), jnp.float32),
        jnp.zeros((lists_here,), jnp.float32),
    )
    final_state, unused = lax.scan(
        accumulate, start_state, (row_blocks, slot_blocks, weight_blocks)
    )
    return final_state


def shards_general(vectors, list_ids, spill_weight, list_pos, old_centroids):
    owners = lax.axis_size("grp")
    row_count, slot_count = list_ids.shape
    feature_dim = vectors.shape[1]
    lists_here = old_centroids.shape[0]
    cap_slots = row_count * slot_count // (2 * owners)
    seat_total = owners * cap_slots
    pair_count = row_count * slot_count
    is_live = list_ids >= 0
    places = jnp.where(is_live, list_pos[jnp.maximum(list_ids, 0)], 0)
    target = jnp.where(is_live, places // lists_here, owners).reshape(-1)
    sorted_order = jnp.argsort(target, stable=True)
    ranked = target[sorted_order]
    counts = jnp.sum(
        (target[:, None] == jnp.arange(owners, dtype=jnp.int32)[None, :]).astype(jnp.int32), axis=0
    )
    starts = jnp.concatenate([jnp.cumsum(counts) - counts, jnp.zeros((1,), jnp.int32)])
    within = jnp.arange(pair_count, dtype=jnp.int32) - starts[ranked]
    seat_sorted = jnp.where(ranked < owners, ranked * cap_slots + within, seat_total)
    seat_index = jnp.zeros((pair_count,), jnp.int32).at[sorted_order].set(seat_sorted)
    pair_of_seat = (
        jnp.full((seat_total,), -1, jnp.int32)
        .at[seat_index]
        .set(jnp.arange(pair_count, dtype=jnp.int32), mode="drop")
    )
    filled = pair_of_seat >= 0
    pair_safe = jnp.maximum(pair_of_seat, 0)
    source_row = jnp.where(filled, pair_safe // slot_count, -1)
    send_rows = pick_rows(vectors, source_row)
    local_flat = (places % lists_here).reshape(-1)
    weight_flat = spill_weight.reshape(-1)
    tag_out = jnp.where(filled, local_flat[pair_safe] + 1, 0)
    weight_out = jnp.where(filled, weight_flat[pair_safe], 0)
    send_meta = jnp.stack([tag_out // 128, tag_out % 128, weight_out], axis=-1).astype(jnp.bfloat16)
    got_rows, got_meta = (
        lax.all_to_all(
            send_rows.reshape(owners, cap_slots, feature_dim),
            "grp",
            split_axis=0,
            concat_axis=0,
            tiled=True,
        ),
        lax.all_to_all(
            send_meta.reshape(owners, cap_slots, 3), "grp", split_axis=0, concat_axis=0, tiled=True
        ),
    )
    got_rows = got_rows.reshape(seat_total, feature_dim)
    got_meta = got_meta.reshape(seat_total, 3)
    seat_live, seat_row, seat_weight = decode_meta(got_meta)
    weighted_sums, totals = owner_sums(got_rows, seat_row, seat_weight, old_centroids, lists_here)
    weighted_sums, totals = lax.psum((weighted_sums, totals), "rep")
    refined = (old_centroids + weighted_sums) / (1.0 + totals[:, None])
    block_rows = math.gcd(512, seat_total)
    block_count = seat_total // block_rows
    row_blocks = got_rows.reshape(block_count, block_rows, feature_dim)
    slot_blocks = seat_row.reshape(block_count, block_rows)

    def distance(piece_item):
        rows_in, slot_in = piece_item
        row_values = rows_in.astype(jnp.float32)
        return jnp.sum((row_values - pick_block(refined, slot_in)) ** 2, axis=-1) / D

    owner_dist = lax.map(distance, (row_blocks, slot_blocks)).reshape(owners, cap_slots)
    seat_dist = lax.all_to_all(owner_dist, "grp", split_axis=0, concat_axis=0, tiled=True).reshape(
        seat_total
    )
    picked = seat_dist[jnp.minimum(seat_index, seat_total - 1)].reshape(row_count, slot_count)
    new_dist = jnp.where(is_live, picked, jnp.float32(0.0))
    return (refined, new_dist)


MESH = pl.DeviceIdType.MESH
LANES = 128
LINE = 4
STORES = 1
F32 = jnp.float32
BF16 = jnp.bfloat16


def xor_index(a, b_const, bits):
    out = 0
    for i in range(bits):
        bit = (a // (1 << i)) % 2
        out = out + ((1 - bit) if (b_const >> i) & 1 else bit) * (1 << i)
    return out


def split_two(x):
    hi = x.astype(BF16)
    return hi, (x - hi.astype(F32)).astype(BF16)


def dot(a, b):
    return jnp.dot(a, b, preferred_element_type=F32)


def iota(shape, dim):
    return lax.broadcasted_iota(jnp.int32, shape, dim)


def take_lanes(line, at):
    wide = jnp.broadcast_to(line, at.shape)
    return jnp.take_along_axis(wide, at, axis=1, mode="promise_in_bounds")


def line_kernel(
    owners, cap,
    vec_hbm, ids_hbm, weight_hbm, pos_hbm, cent_hbm,
    refined_ref, dist_ref,
    ints, vec_other, cent, cent_cat, raw_in, meta_in, seat_keep, send_buf, send_near, rows, codes,
    masks, placed, sq_own, sq_sib, acc, tot, back_send, back,
    l_sem, s_own, s_meta, r_half, r_raw, r_meta, s_row, r_row, s_code, r_code, s_sq, r_sq, s_back, r_back, s_ref, r_ref, s_near, first, second,
):
    me = lax.axis_index("grp")
    rep = lax.axis_index("rep")
    slot_count, row_count = seat_keep.shape
    lists_here, half = cent.shape
    table_rows = pos_hbm.shape[0]
    plane = owners // LINE
    pbits = plane.bit_length() - 1
    z = me // plane
    p = me % plane
    mid = ((z + 1) // 2) % 2
    near = z + 1 - 2 * (z % 2)
    inner = LINE - 1 - z
    cross = (z + 2) % LINE
    z_of = [z, near, mid * inner + (1 - mid) * cross, mid * cross + (1 - mid) * inner]
    xz_of = [0, 1, 2 + mid, 3 - mid]
    rep_of = [rep, 1 - rep]
    mine = pl.ds(pl.multiple_of(rep * half, LANES), half)
    theirs = pl.ds(pl.multiple_of((1 - rep) * half, LANES), half)

    def at(place, xp):
        return place * plane + xor_index(p, xp, pbits)

    barrier = pltpu.get_barrier_semaphore()

    def greet(place, xp, r):
        pl.semaphore_signal(barrier, inc=1, device_id={"grp": at(place, xp), "rep": r}, device_id_type=MESH)

    greet(near, 0, 0)
    greet(near, 0, 1)

    @pl.when(mid == 1)
    def _():
        greet(inner, 0, 0)
        greet(inner, 0, 1)

    for i in range(pbits):
        greet(z, 1 << i, rep)
    greet(z, 0, 1 - rep)

    local = [
        pltpu.make_async_copy(vec_hbm.at[:, mine], raw_in.at[0, 0], l_sem.at[0]),
        pltpu.make_async_copy(vec_hbm.at[:, theirs], vec_other, l_sem.at[1]),
        pltpu.make_async_copy(ids_hbm, ints.at[pl.ds(0, slot_count)], l_sem.at[2]),
        pltpu.make_async_copy(weight_hbm, ints.at[pl.ds(slot_count, slot_count)], l_sem.at[2]),
        pltpu.make_async_copy(pos_hbm, ints.at[pl.ds(2 * slot_count, table_rows)], l_sem.at[2]),
        pltpu.make_async_copy(cent_hbm.at[:, mine], cent, l_sem.at[3]),
    ]
    for copy in local:
        copy.start()

    def tell(semaphore, steps):
        for j in steps:
            pl.semaphore_signal(semaphore, inc=1, device_id={"grp": at(z, j), "rep": rep}, device_id_type=MESH)

    def remote(src, dst, send, recv, place, xp, r):
        return pltpu.make_async_remote_copy(
            src_ref=src, dst_ref=dst, send_sem=send, recv_sem=recv,
            device_id={"grp": at(place, xp), "rep": r}, device_id_type=MESH,
        )

    own_place = [z, near, inner]
    others = pl.ds(1, plane - 1)

    own_half = row_count // 2

    def row_half(ref, c):
        return ref.at[pl.ds(c * own_half, own_half)]

    def own_raw(s, f):
        src = raw_in.at[0, 0] if f == 0 else vec_other
        to = raw_in.at[s, f]
        if s != 1:
            return [remote(src, to, s_own.at[s // 2], r_raw.at[s, f], own_place[s], 0, rep_of[f])]
        return [
            remote(
                row_half(src, c), row_half(to, c), s_own.at[0], r_half.at[f] if c == 0 else r_raw.at[1, f],
                near, 0, rep_of[f],
            )
            for c in range(2)
        ]

    def own_meta(s, f):
        return remote(
            meta_in.at[0, 0], meta_in.at[s, f], s_meta.at[s // 2], r_meta.at[s, f], own_place[s], 0, rep_of[f]
        )

    def forward(f, c):
        if c is None:
            return remote(meta_in.at[1, f], meta_in.at[3, f], s_meta.at[1], r_meta.at[3, f], inner, 0, rep)
        src, to = row_half(raw_in.at[1, f], c), row_half(raw_in.at[3, f], c)
        return remote(src, to, s_own.at[1], r_raw.at[3, f], inner, 0, rep)

    def row_copy(s, f, j):
        return remote(send_buf.at[s, f, j], rows.at[s, f, j], s_row, r_row.at[s], z, j, rep)

    def code_copy(s, f, j):
        src = meta_in.at[s, f, slot_count + xz_of[s]]
        return remote(src, codes.at[s, f, j], s_code, r_code.at[s], z, j, rep)

    def near_row_copy(s, f, j):
        return remote(send_near.at[s - 2, f, j], rows.at[s, f, j], s_own.at[1], r_row.at[s], near, j, rep)

    def near_code_copy(s, f, j):
        src = meta_in.at[s, f, slot_count + s]
        return remote(src, codes.at[s, f, j], s_near, r_code.at[s], near, j, rep)

    def sq_copy(s):
        return remote(sq_own.at[s], sq_sib.at[s], s_sq, r_sq.at[s], z, 0, 1 - rep)

    def back_copy(s, f, j):
        to = back.at[(xz_of[s] * plane + j) * 2 + f]
        return remote(back_send.at[s, f], to, s_back, r_back, z_of[s], j, rep_of[f])

    def arrived(ref, sem):
        pltpu.make_async_copy(ref, ref, sem).wait()

    ref_copy = remote(refined_ref.at[:, mine], refined_ref.at[:, mine], s_ref, r_ref, z, 0, 1 - rep)
    ref_wait = remote(refined_ref.at[:, theirs], refined_ref.at[:, theirs], s_ref, r_ref, z, 0, 1 - rep)

    pl.semaphore_wait(barrier, pbits + 3 + 2 * mid)
    def own_to(f):
        for copy in own_raw(1, f):
            copy.start()

        @pl.when(mid == 1)
        def _():
            for copy in own_raw(2, f):
                copy.start()

    tell(first, [1 << i for i in range(pbits)])
    local[0].wait()
    own_to(0)
    local[1].wait()
    for copy in own_raw(0, 1):
        copy.start()
    pltpu.make_async_copy(ints, ints, l_sem.at[2]).wait()
    raw_ids = ints[pl.ds(0, slot_count)]
    weights = ints[pl.ds(slot_count, slot_count)]
    table = ints[pl.ds(2 * slot_count, table_rows)]
    live = raw_ids >= 0
    safe_ids = jnp.maximum(raw_ids, 0)
    place = jnp.zeros((slot_count, row_count), jnp.int32)
    for r in range(table_rows):
        taken = take_lanes(table[r : r + 1], safe_ids % LANES)
        place = jnp.where(safe_ids // LANES == r, taken, place)
    owner = place // lists_here
    to_z, to_p = owner // plane, owner % plane

    def xor_two(a, b, bits):
        out = 0
        for i in range(bits):
            out = out + ((a // (1 << i) + b // (1 << i)) % 2) * (1 << i)
        return out

    turned = xor_two(to_z, z, 2) * plane + xor_two(to_p, p, pbits)
    turned = jnp.where(live, turned, -1)
    code = ((place % lists_here) * 8 + weights).astype(F32)
    square = (LANES, LANES)
    lane = iota(square, 1)
    sub = iota(square, 0)
    member = jnp.concatenate([(turned == o).astype(F32) for o in range(owners)], axis=0).astype(BF16)
    earlier = (sub < lane).astype(F32).astype(BF16)
    same_owner = sub // slot_count == lane // slot_count
    prior = (same_owner & (lane < sub)).astype(F32).astype(BF16)
    before = dot(prior, member).astype(BF16)
    rank_all = dot(member, earlier) + dot(before, jnp.ones(square, BF16))
    rank = jnp.zeros((slot_count, row_count), F32)
    for o in range(owners):
        rank = jnp.where(turned == o, rank_all[o * slot_count : (o + 1) * slot_count], rank)
    seat = jnp.where(live, turned.astype(F32) * cap + rank, -1.0)
    seat_keep[...] = seat
    for k in range(slot_count):
        meta_in[0, 0, k] = seat[k : k + 1]
    eye = sub == lane

    def to_row(col):
        return jnp.sum(jnp.where(eye, col, 0.0), axis=0, keepdims=True)

    def to_col(row):
        return jnp.sum(jnp.where(eye, row, 0.0), axis=1, keepdims=True)

    for g in range(LINE):
        q = (sub + g * LANES).astype(F32)
        found = jnp.zeros(square, F32)
        for k in range(slot_count):
            found = found + jnp.where(seat[k : k + 1] == q, code[k : k + 1], 0.0)
        meta_in[0, 0, slot_count + g] = to_row(jnp.sum(found, axis=1, keepdims=True))

    for f in range(2):
        own_meta(1, f).start()

    @pl.when(mid == 1)
    def _():
        for f in range(2):
            own_meta(2, f).start()

    own_to(1)
    own_meta(0, 1).start()

    def picked_rows(s, f, xz):
        q = (sub + xz * LANES).astype(F32)
        chosen = jnp.zeros(square, F32)
        for k in range(slot_count):
            chosen = chosen + (meta_in[s, f, k] == q).astype(F32)
        return dot(chosen.astype(BF16), raw_in[s, f]).astype(BF16).reshape(plane, cap, half)

    def receive(s, f, passed_on=False):
        arrived(meta_in.at[s, f], r_meta.at[s, f])
        if passed_on:
            forward(f, None).start()
        if s == 1:
            arrived(row_half(raw_in.at[1, f], 0), r_half.at[f])
            if passed_on:
                forward(f, 0).start()
            arrived(row_half(raw_in.at[1, f], 1), r_raw.at[1, f])
            if passed_on:
                forward(f, 1).start()
        else:
            arrived(raw_in.at[s, f], r_raw.at[s, f])

    def to_near(s, f):
        for j in reversed(range(plane)):
            near_code_copy(s, f, j).start()
        send_near[s - 2, f] = picked_rows(s, f, s)
        for j in reversed(range(plane)):
            near_row_copy(s, f, j).start()

    def to_plane(s, f):
        if (s, f) != (0, 0):
            for j in reversed(range(1, plane)):
                code_copy(s, f, j).start()
        picked = picked_rows(s, f, xz_of[s])
        send_buf[s, f] = picked
        if (s, f) == (0, 0):
            pl.semaphore_wait(first, pbits)
            tell(second, [1])
            for j in reversed(range(1, plane)):
                code_copy(s, f, j).start()
        for j in reversed(range(1, plane)):
            row_copy(s, f, j).start()
        rows[s, f, 0] = picked[0]
        codes[s, f, 0] = meta_in[s, f, slot_count + xz_of[s]]

    lane_row = iota((1, LANES), 1)

    def code_row(s, f):
        out = codes[s, f, 0]
        for j in range(1, plane):
            out = jnp.where(lane_row // cap == j, codes[s, f, j], out)
        return out

    def halves(x):
        return x[:, :half] + x[:, half : 2 * half]

    def lane_parts(x):
        out = x[:, :LANES]
        for i in range(1, half // LANES):
            out = out + x[:, i * LANES : (i + 1) * LANES]
        return out

    def got_rows(s):
        return rows[s].reshape(2 * LANES, half).astype(F32)

    centres = {}

    def near_part(s, picked_here=True):
        before_rows(s, picked_here)
        after_rows(s, picked_here)

    def before_rows(s, picked_here=True):
        arrived(codes.at[s, :, others] if picked_here else codes.at[s], r_code.at[s])
        for f in range(2):
            row = code_row(s, f)
            wide = to_col(row).astype(jnp.int32) // 8
            masks[s, pl.ds(f * LANES, LANES)] = (
                (wide == iota((LANES, lists_here), 1)).astype(F32).astype(BF16)
            )
            placed[s, :, pl.ds(f * LANES, LANES)] = (
                (row.astype(jnp.int32) // 8 == iota((lists_here, LANES), 0)).astype(F32).astype(BF16)
            )
        centres[s] = halves(dot(masks[s], cent_cat[...]))

    def after_rows(s, picked_here=True):
        arrived(rows.at[s, :, others] if picked_here else rows.at[s], r_row.at[s])
        diff = got_rows(s) - centres[s]
        sq_own[s] = lane_parts(diff * diff)
        sq_copy(s).start()

    def with_share_of(s):
        weight = jnp.concatenate(
            [to_col((code_row(s, f).astype(jnp.int32) % 8).astype(F32)) for f in range(2)], axis=0
        )
        got = got_rows(s)
        sq_copy(s).wait_recv()
        swapped = jnp.concatenate([sq_sib[s, LANES:], sq_sib[s, :LANES]], axis=0)
        sq = jnp.sum(sq_own[s] + swapped, axis=1, keepdims=True)
        share = jnp.broadcast_to(weight / (1.0 + sq / (2 * half)), (2 * LANES, LANES))
        share_hi, share_lo = split_two(share)
        sv_hi, sv_lo = split_two(jnp.concatenate([share] * (half // LANES), axis=1) * got)
        added = dot(placed[s], jnp.concatenate([sv_hi, sv_lo, share_hi, share_lo], axis=1))
        sums = halves(added)
        counts = added[:, 2 * half : 2 * half + LANES] + added[:, 2 * half + LANES :]
        if s == 0:
            return cent[...] + sums, counts
        return acc[...] + sums, tot[...] + counts

    def far_part(s):
        acc[...], tot[...] = with_share_of(s)

    to_plane(0, 0)
    local[5].wait()
    hi, lo = split_two(cent[...])
    cent_cat[:, pl.ds(0, half)] = hi
    cent_cat[:, pl.ds(half, half)] = lo
    receive(0, 1)
    to_plane(0, 1)

    def follow(steps):
        for step, args in steps:
            step(*args)

    @pl.when(mid == 1)
    def _():
        pl.semaphore_wait(second, 1)
        follow([
            (receive, (1, 0, True)), (receive, (2, 0)), (to_near, (2, 0)), (receive, (1, 1, True)), (receive, (2, 1)), (to_near, (2, 1)),
            (to_plane, (1, 0)), (to_plane, (2, 0)), (to_plane, (1, 1)), (to_plane, (2, 1)), (near_part, (0,)),
            (receive, (3, 0)), (to_near, (3, 0)), (to_plane, (3, 0)), (receive, (3, 1)), (to_near, (3, 1)), (to_plane, (3, 1)),
            (far_part, (0,)), (near_part, (1,)), (near_part, (2,)), (far_part, (1,)), (near_part, (3,)), (far_part, (2,)),
        ])

    @pl.when(mid == 0)
    def _():
        pl.semaphore_wait(second, 1)
        follow([
            (receive, (1, 0)), (to_plane, (1, 0)), (receive, (1, 1)), (to_plane, (1, 1)), (near_part, (0,)), (near_part, (1,)),
            (far_part, (0,)), (far_part, (1,)),
            (near_part, (2, False)), (before_rows, (3, False)), (far_part, (2,)), (after_rows, (3, False)),
        ])

    sums, counts = with_share_of(LINE - 1)
    scale = 1.0 / (1.0 + counts)
    refined = sums * jnp.concatenate([scale] * (half // LANES), axis=1)
    refined_ref[:, mine] = refined
    hi, lo = split_two(refined)
    cent_cat[:, pl.ds(0, half)] = hi
    cent_cat[:, pl.ds(half, half)] = lo

    for s in reversed(range(LINE)):
        diff = got_rows(s) - halves(dot(masks[s], cent_cat[...]))
        value = jnp.sum(lane_parts(diff * diff), axis=1, keepdims=True) / (2 * half)
        for f in range(2):
            row = to_row(value[f * LANES : (f + 1) * LANES])
            back_send[s, f] = row
            for j in reversed(range(plane)):
                if (s, f, j) != (0, 0, 0):
                    back_copy(s, f, j).start()
            if (s, f) == (0, 0):
                back[0] = row
        if s == 2:
            ref_copy.start()

    seats = seat_keep[...].astype(jnp.int32)
    lanes_at = jnp.maximum(seats, 0) % LANES
    out = jnp.zeros((slot_count, row_count), F32)
    arrived(back.at[pl.ds(1, 2 * owners - 1)], r_back)
    for x in range(LINE):
        line = jnp.zeros((1, LANES), F32)
        for j in range(plane):
            first = (x * plane + j) * 2
            line = jnp.where(lane_row // cap == j, back[first] + back[first + 1], line)
        taken = take_lanes(line, lanes_at)
        out = jnp.where((seats >= 0) & (seats // LANES == x), taken, out)
    dist_ref[...] = out

    ref_wait.wait_recv()
    ref_copy.wait_send()
    arrived(raw_in.at[pl.ds(0, 3), 0], s_own.at[0])
    arrived(meta_in.at[pl.ds(0, 3), 0], s_meta.at[0])

    @pl.when(mid == 1)
    def _():
        arrived(raw_in, s_own.at[1])
        arrived(meta_in.at[pl.ds(0, 2)], s_meta.at[1])
        arrived(rows.at[:, :, others], s_row)
        arrived(codes.at[:, :, others], s_code)
        arrived(codes.at[pl.ds(2, 2)], s_near)

    @pl.when(mid == 0)
    def _():
        arrived(rows.at[pl.ds(0, 2), :, others], s_row)
        arrived(codes.at[pl.ds(0, 2), :, others], s_code)

    arrived(sq_own, s_sq)
    arrived(back.at[pl.ds(1, 2 * owners - 1)], s_back)


def store_kernel(refined_ref, dist_ref, refined_out, dist_out, sems):
    part = refined_ref.shape[0] // STORES
    copies = [pltpu.make_async_copy(dist_ref, dist_out, sems.at[STORES])]
    for i in range(STORES):
        span = pl.ds(i * part, part)
        copies.append(pltpu.make_async_copy(refined_ref.at[span], refined_out.at[span], sems.at[i]))
    for copy in copies:
        copy.start()
    for copy in copies:
        copy.wait()


def shards(vectors, list_ids, spill_weight, list_pos, old_centroids):
    owners = lax.axis_size("grp")
    row_count, slot_count = list_ids.shape
    feature_dim = vectors.shape[1]
    lists_here = old_centroids.shape[0]
    cap = row_count * slot_count // (2 * owners)
    plane = owners // LINE
    fits = (
        row_count == LANES and slot_count == 8 and owners * cap == LINE * LANES and plane == 4
        and owners * slot_count == LANES and cap % 16 == 0 and lax.axis_size("rep") == 2
        and lists_here % LANES == 0 and feature_dim % (2 * LANES) == 0 and list_pos.shape[0] % LANES == 0
    )
    if not fits:
        return shards_general(vectors, list_ids, spill_weight, list_pos, old_centroids)
    half = feature_dim // 2
    table_rows = list_pos.shape[0] // LANES
    meta_rows = slot_count + LINE
    vmem = pl.BlockSpec(memory_space=pltpu.VMEM)
    hbm = pl.BlockSpec(memory_space=pl.ANY)
    dma = pltpu.SemaphoreType.DMA
    refined, dist = pl.pallas_call(
        functools.partial(line_kernel, owners, cap),
        out_shape=(
            pltpu.VMEM((lists_here, feature_dim), F32),
            pltpu.VMEM((slot_count, row_count), F32),
        ),
        in_specs=[hbm] * 5,
        out_specs=(vmem, vmem),
        scratch_shapes=[
            pltpu.VMEM((2 * slot_count + table_rows, LANES), jnp.int32),
            pltpu.VMEM((row_count, half), BF16),
            pltpu.VMEM((lists_here, half), F32),
            pltpu.VMEM((lists_here, feature_dim), BF16),
            pltpu.VMEM((LINE, 2, row_count, half), BF16),
            pltpu.VMEM((LINE, 2, meta_rows, 1, LANES), F32),
            pltpu.VMEM((slot_count, row_count), F32),
            pltpu.VMEM((LINE, 2, plane, cap, half), BF16),
            pltpu.VMEM((2, 2, plane, cap, half), BF16),
            pltpu.VMEM((LINE, 2, plane, cap, half), BF16),
            pltpu.VMEM((LINE, 2, plane, 1, LANES), F32),
            pltpu.VMEM((LINE, 2 * LANES, lists_here), BF16),
            pltpu.VMEM((LINE, lists_here, 2 * LANES), BF16),
            pltpu.VMEM((LINE, 2 * LANES, LANES), F32),
            pltpu.VMEM((LINE, 2 * LANES, LANES), F32),
            pltpu.VMEM((lists_here, half), F32),
            pltpu.VMEM((lists_here, LANES), F32),
            pltpu.VMEM((LINE, 2, 1, LANES), F32),
            pltpu.VMEM((2 * owners, 1, LANES), F32),
            dma((4,)),
            dma((2,)), dma((2,)), dma((2,)), dma((LINE, 2)), dma((LINE, 2)),
            dma(()), dma((LINE,)), dma(()), dma((LINE,)), dma(()), dma((LINE,)),
            dma(()), dma(()), dma(()), dma(()), dma(()), pltpu.SemaphoreType.REGULAR,
            pltpu.SemaphoreType.REGULAR,
        ],
        compiler_params=pltpu.CompilerParams(collective_id=0, has_side_effects=True),
    )(vectors, list_ids.T, spill_weight.T, list_pos.reshape(-1, LANES), old_centroids)
    refined, dist = pl.pallas_call(
        store_kernel,
        out_shape=(
            pltpu.HBM((lists_here, feature_dim), F32),
            pltpu.HBM((slot_count, row_count), F32),
        ),
        in_specs=[vmem, vmem],
        out_specs=(hbm, hbm),
        scratch_shapes=[dma((STORES + 1,))],
    )(*(pltpu.with_memory_space_constraint(x, pltpu.MemorySpace.VMEM) for x in (refined, dist)))
    return refined, dist.T


def solution(mesh):
    return jax.shard_map(
        shards,
        mesh=mesh,
        in_specs=(
            P(("grp", "rep"), None),
            P(("grp", "rep"), None),
            P(("grp", "rep"), None),
            P(),
            P("grp", None),
        ),
        out_specs=(P("grp", None), P(("grp", "rep"), None)),
        check_vma=False,
    )
```
